32 devices in a mesh: wide: 4 (over y, core), narrow: 4 (over z), depth: 2 (over x).
Axes of the slice: x: 2, y: 2, z: 4, core: 2. Of those that a mesh axis runs over, the one named last changes fastest.
Arguments:
- hidden_state: bfloat16 [16, 4096], P(('wide', 'depth')), may hold values from -6 to 6
- query_weight: bfloat16 [4096, 4096], P('depth', 'narrow'), may hold values from -0.09375 to 0.09375
- output_weight: bfloat16 [4096, 4096], P('narrow'), may hold values from -0.09375 to 0.09375
- cache_keys: bfloat16 [16, 512, 4096], P(('wide', 'depth'), None, 'narrow'), may hold values from -128 to 128
- cache_values: bfloat16 [16, 512, 4096], P(('wide', 'depth'), None, 'narrow'), may hold values from -12 to 12
- enc_blocks: int32 [16], replicated, may hold values from 1 to 4
- cache_slot: int32 [16], replicated, may hold values from 0 to 15, as said below
Outputs:
- attended: bfloat16 [16, 4096], P(('wide', 'depth'), 'narrow')
The draws below stay inside these ranges and needn't reach their ends.
Inputs may be any that keep to these rules, and one draw needn't show every extreme that they name: Request r attends to the first 128 * enc_blocks[r] rows of its cache slot. Every slot holds exactly one request, and r and cache_slot[r] agree in their value of (index // 2) % 2.
All inputs are finite; a program needn't handle non-finite values.
Results may differ from the reference program's by a relative error of at most 0.012.
The reference program's roundings to bfloat16 on the way (of `normed`, `queries`, `shares` and `context`) count: a program that leaves them out, or rounds other values in their place, can miss the bound.
Values may be sent and summed in bfloat16 or wider, within the bound.
No kernel may reach another device: no remote copies, remote signals or barrier semaphores. Data moves between devices by JAX's collectives and lax.ppermute only.
A program may use at most 64 MiB of HBM per device.

```python
import jax
import jax.numpy as jnp
from jax import lax

D = 4096
HEADS = 64
HDIM = 64
REQ_DEV = 2
LMAX = 512
BLOCK = 128
BLOCKS = 4
OWNERS = 4
HALVES = 2
REQUESTS = 16


def draw_cache_keys(key, part):
    arr_shape = (REQUESTS, LMAX, HEADS * HDIM)
    key_base = jax.random.fold_in(key, 0)
    return jnp.clip(jax.random.normal(key_base, arr_shape, jnp.float32) * 0.3, -2.0, 2.0).astype(jnp.bfloat16)


def draw_cache_slot(key, part):
    combos = OWNERS * REQ_DEV
    subkeys = jax.random.split(jax.random.fold_in(key, 7), HALVES)
    orders = jax.vmap(lambda subkey: jax.random.permutation(subkey, combos))(subkeys)
    request = jnp.arange(REQUESTS, dtype=jnp.int32)
    depth_of = request // REQ_DEV % HALVES
    combo_at = request // (REQ_DEV * HALVES) * REQ_DEV + request % REQ_DEV
    target = orders[depth_of, combo_at].astype(jnp.int32)
    return ((target // REQ_DEV * HALVES + depth_of) * REQ_DEV + target % REQ_DEV).astype(jnp.int32)


def touch_ends(entries, rng, least, top_value):
    longest = entries.shape.index(max(entries.shape))
    spots = []
    for shift in (0, 1):
        where = [jax.random.randint(jax.random.fold_in(rng, axis), (), 0, length) for axis, length in enumerate(entries.shape)]
        where[longest] = (where[longest] + shift) % entries.shape[longest]
        spots.append(tuple(where))
    return entries.at[spots[0]].set(least).at[spots[1]].set(top_value)


def level_of(stream_key, shape, cuts, least, high):
    factor_of, own = 1.0, jax.random.fold_in(stream_key, 6)
    for dim, shards_of in cuts:
        heights = jnp.exp(jax.random.uniform(jax.random.fold_in(own, dim), (shards_of,), jnp.float32, least / len(cuts), high / len(cuts)))
        factor_of = factor_of * jnp.repeat(heights, shape[dim] // shards_of).reshape([-1 if axis == dim else 1 for axis in range(len(shape))])
    return factor_of


def scatter_about(own_key, dims, deviation, most, cuts=(), kind=jnp.bfloat16):
    entries = jax.random.normal(own_key, dims, jnp.float32) * deviation
    if len(cuts) > 0:
        entries = level_of(own_key, dims, cuts, -0.22, 0.18) * entries
    return jnp.clip(entries, min=-most, max=most).astype(kind)


def setup_inputs(seed: int = 0) -> dict:
    key_list = jax.random.split(jax.random.key(seed), 8)
    hidden_state = scatter_about(key_list[0], (REQUESTS, D), 1.0, 6.0, ((0, 8),))
    query_weight = scatter_about(key_list[1], (D, HEADS * HDIM), D ** -0.5, 0.09375, ((0, 2), (1, 4)))
    output_weight = scatter_about(key_list[2], (HEADS * HDIM, D), (HEADS * HDIM) ** -0.5, 0.09375, ((0, 4),))
    cache_keys = draw_cache_keys(jax.random.fold_in(key_list[7], 71), 0)
    cache_values = scatter_about(key_list[4], (REQUESTS, LMAX, HEADS * HDIM), 2.0, 12.0, ((0, 8), (2, 4)))
    enc_blocks = touch_ends(jax.random.randint(key_list[5], (REQUESTS,), 1, BLOCKS + 1), jax.random.fold_in(key_list[5], 1), 1, BLOCKS).astype(jnp.int32)
    cache_slot = draw_cache_slot(jax.random.fold_in(key_list[7], 71), 0)
    return dict(hidden_state=hidden_state, query_weight=query_weight, output_weight=output_weight, cache_keys=cache_keys, cache_values=cache_values, enc_blocks=enc_blocks, cache_slot=cache_slot)


def attend_one(packed, cache_keys, cache_values, positions):
    query_row, slot_row, block_count = packed
    key_rows = lax.dynamic_index_in_dim(cache_keys, slot_row.astype(jnp.int32), 0, keepdims=False)
    value_rows = lax.dynamic_index_in_dim(cache_values, slot_row.astype(jnp.int32), 0, keepdims=False)
    query_heads = query_row.reshape(HEADS, HDIM).astype(jnp.float32)
    key_heads = key_rows.reshape(LMAX, HEADS, HDIM).astype(jnp.float32)
    value_heads = value_rows.reshape(LMAX, HEADS, HDIM).astype(jnp.float32)
    scores = jnp.einsum('hd,lhd->hl', query_heads, key_heads)
    usable = positions < block_count.astype(jnp.int32) * BLOCK
    scores = jnp.where(usable[None, :], scores, jnp.float32(-1e+30))
    row_top = lax.optimization_barrier(jnp.max(scores, axis=-1, keepdims=True))
    raised = jnp.exp(scores - row_top)
    shares = (raised / lax.optimization_barrier(jnp.sum(raised, axis=-1, keepdims=True))).astype(jnp.bfloat16)
    context = jnp.einsum('hl,lhd->hd', shares.astype(jnp.float32), value_heads)
    return context.reshape(HEADS * HDIM).astype(jnp.bfloat16)

def reference(hidden_state, query_weight, output_weight, cache_keys, cache_values, enc_blocks, cache_slot):
    widened = hidden_state.astype(jnp.float32)
    mean_square = lax.optimization_barrier(jnp.mean(widened * widened, axis=-1, keepdims=True))
    normed = (widened * lax.rsqrt(mean_square + 1e-06)).astype(jnp.bfloat16)
    queries = jnp.dot(normed, query_weight, preferred_element_type=jnp.float32).astype(jnp.bfloat16)
    positions = jnp.arange(LMAX, dtype=jnp.int32)
    context = lax.map(lambda packed: attend_one(packed, cache_keys, cache_values, positions), (queries, cache_slot, enc_blocks))
    return jnp.dot(context, output_weight, preferred_element_type=jnp.float32).astype(jnp.bfloat16)
```

```python
import jax
import jax.numpy as jnp
from jax import lax
from jax.experimental import pallas as pl
from jax.experimental.pallas import tpu as pltpu
from jax.sharding import PartitionSpec as P

HDIM = 64
BLOCK = 128

VMEM = pl.BlockSpec(memory_space=pltpu.VMEM)
SMEM = pl.BlockSpec(memory_space=pltpu.SMEM)


def request_of(slot_ref, slot, lead):
    found = jnp.int32(0)
    for r in lead:
        found = jnp.where(slot_ref[r] == slot, jnp.int32(r), found)
    return found


def norm_kernel(hidden_ref, own_ref, other_ref):
    half = own_ref.shape[1]
    at_depth = lax.axis_index("depth")
    widened = hidden_ref[...].astype(jnp.float32)
    mean_square = jnp.mean(widened * widened, axis=-1, keepdims=True)
    normed = widened * lax.rsqrt(mean_square + 1e-06)
    low, high = normed[:, :half], normed[:, half:]
    first = at_depth == 0
    own_ref[...] = jnp.where(first, low, high).astype(jnp.bfloat16)
    other_ref[...] = jnp.where(first, high, low).astype(jnp.bfloat16)


def query_kernel(sizes, slot_ref, *refs):
    wide, halves, rows = sizes
    pieces = len(refs) - 1 - 4 - 2
    piece_refs, weight_ref = refs[:pieces], refs[pieces]
    out_refs = refs[pieces + 1 : pieces + 5]
    rows_ref, sums_ref = refs[pieces + 5 :]
    at_wide, at_depth = lax.axis_index("wide"), lax.axis_index("depth")
    for k, piece in enumerate(piece_refs):
        rows_ref[k * rows : (k + 1) * rows, :] = piece[...].astype(jnp.float32)
    sums_ref[...] = jnp.dot(
        rows_ref[...].astype(jnp.bfloat16), weight_ref[...], preferred_element_type=jnp.float32
    )
    total = wide * halves * rows
    for k, out in enumerate(out_refs):
        flip_wide, flip_depth = k // 2, k % 2
        peer_wide, peer_depth = at_wide ^ flip_wide, at_depth ^ flip_depth
        for j in range(rows):
            slot = (peer_wide * halves + peer_depth) * rows + j
            r = request_of(slot_ref, slot, range(total))
            from_wide = r // (rows * halves) ^ at_wide
            from_depth = (r // rows) % halves ^ at_depth
            here = (from_wide & 1) == 0
            place = ((from_wide >> 1) * halves + from_depth) * rows + r % rows
            row = sums_ref[pl.ds(place, 1), :]
            out[j : j + 1, :] = jnp.where(here, row, 0.0)


def attend_kernel(sizes, slot_ref, blocks_ref, *refs):
    wide, narrow, halves, rows = sizes
    parts, (keys_ref, values_ref, weight_ref, out_ref) = refs[:4], refs[4:]
    at_wide, at_depth = lax.axis_index("wide"), lax.axis_index("depth")
    cache_len, features = keys_ref.shape[1:]
    heads = features // HDIM
    total = wide * halves * rows
    queries = (parts[0][...] + parts[2][...]) + (parts[1][...] + parts[3][...])
    of_head = (
        lax.broadcasted_iota(jnp.int32, (heads, features), 1) // HDIM
        == lax.broadcasted_iota(jnp.int32, (heads, features), 0)
    )
    positions = lax.broadcasted_iota(jnp.int32, (heads, cache_len), 1)
    contexts = []
    for j in range(rows):
        slot = (at_wide * halves + at_depth) * rows + j
        count = jnp.int32(0)
        for r in range(total):
            count = jnp.where(slot_ref[r] == slot, blocks_ref[r], count)
        spread = jnp.where(of_head, queries[j : j + 1, :], 0.0).astype(jnp.bfloat16)
        scores = lax.dot_general(
            spread, keys_ref[j], (((1,), (1,)), ((), ())), preferred_element_type=jnp.float32
        )
        scores = jnp.where(positions < count * BLOCK, scores, jnp.float32(-1e30))
        row_top = jnp.max(scores, axis=-1, keepdims=True)
        raised = jnp.exp(scores - row_top)
        shares = (raised / jnp.sum(raised, axis=-1, keepdims=True)).astype(jnp.bfloat16)
        mixed = jnp.dot(shares, values_ref[j], preferred_element_type=jnp.float32)
        contexts.append(jnp.sum(jnp.where(of_head, mixed, 0.0), axis=0, keepdims=True))
    padding = jnp.zeros((8 - rows, features), jnp.float32)
    context = jnp.concatenate(contexts + [padding], axis=0).astype(jnp.bfloat16)
    partial = jnp.dot(context, weight_ref[...], preferred_element_type=jnp.float32)
    width = partial.shape[1] // narrow
    for to_wide in range(wide):
        lines = []
        for i in range(rows):
            at = slot_ref[(to_wide * halves + at_depth) * rows + i] - (
                at_wide * halves + at_depth
            ) * rows
            line = jnp.zeros_like(partial[:1])
            for j in range(rows):
                line = jnp.where(at == j, partial[j : j + 1], line)
            lines.append(line)
        block = jnp.concatenate(lines, axis=0).astype(jnp.bfloat16)
        for to_narrow in range(narrow):
            out_ref[to_wide * narrow + to_narrow] = block[
                :, to_narrow * width : (to_narrow + 1) * width
            ]


def sum_kernel(parts_ref, out_ref):
    total = parts_ref[0].astype(jnp.float32)
    for k in range(1, parts_ref.shape[0]):
        total = total + parts_ref[k].astype(jnp.float32)
    out_ref[...] = total.astype(jnp.bfloat16)


def shards(
    hidden_state, query_weight, output_weight, cache_keys, cache_values, enc_blocks, cache_slot
):
    rows = hidden_state.shape[0]
    wide, narrow, halves = (lax.axis_size(name) for name in ("wide", "narrow", "depth"))
    half, features = query_weight.shape
    width = output_weight.shape[1]

    def flipped(x, flip_wide, flip_depth):
        pairs = [
            (w * halves + d, (w ^ flip_wide) * halves + (d ^ flip_depth))
            for w in range(wide)
            for d in range(halves)
        ]
        return lax.ppermute(x, ("wide", "depth"), pairs)

    half_rows = jax.ShapeDtypeStruct((rows, half), jnp.bfloat16)
    own, other = pl.pallas_call(
        norm_kernel,
        out_shape=[half_rows, half_rows],
        in_specs=[VMEM],
        out_specs=[VMEM, VMEM],
    )(hidden_state)
    pieces = []
    for chip in range(wide // 2):
        for flip_depth in range(halves):
            if chip == 0 and flip_depth == 0:
                pieces.append(own)
            else:
                pieces.append(flipped(other if flip_depth else own, chip * 2, flip_depth))
    count = len(pieces) * rows
    sums = jax.ShapeDtypeStruct((rows, features), jnp.float32)
    parts = pl.pallas_call(
        lambda *refs: query_kernel((wide, halves, rows), *refs),
        out_shape=[sums] * 4,
        in_specs=[SMEM] + [VMEM] * (len(pieces) + 1),
        out_specs=[VMEM] * 4,
        scratch_shapes=[
            pltpu.VMEM((count, half), jnp.float32),
            pltpu.VMEM((count, features), jnp.float32),
        ],
    )(cache_slot, *pieces, query_weight)
    arrived = [parts[0]] + [flipped(parts[k], k // 2, k % 2) for k in range(1, 4)]
    spread = pl.pallas_call(
        lambda *refs: attend_kernel((wide, narrow, halves, rows), *refs),
        out_shape=jax.ShapeDtypeStruct((wide * narrow, rows, width // narrow), jnp.bfloat16),
        in_specs=[SMEM, SMEM] + [VMEM] * 7,
        out_specs=VMEM,
    )(cache_slot, enc_blocks, *arrived, cache_keys, cache_values, output_weight)
    gathered = lax.all_to_all(spread, ("wide", "narrow"), 0, 0, tiled=True)
    return pl.pallas_call(
        sum_kernel,
        out_shape=jax.ShapeDtypeStruct((rows, width // narrow), jnp.bfloat16),
        in_specs=[VMEM],
        out_specs=VMEM,
    )(gathered)


def solution(mesh):
    placed = (
        P(("wide", "depth"), None),
        P("depth", "narrow"),
        P("narrow", None),
        P(("wide", "depth"), None, "narrow"),
        P(("wide", "depth"), None, "narrow"),
        P(),
        P(),
    )
    return jax.shard_map(
        shards,
        mesh=mesh,
        in_specs=placed,
        out_specs=P(("wide", "depth"), "narrow"),
        check_vma=False,
    )
```

```python
import jax
import jax.numpy as jnp
from jax import lax
from jax.experimental import pallas as pl
from jax.experimental.pallas import tpu as pltpu
from jax.sharding import PartitionSpec as P

HDIM = 64
BLOCK = 128

MIB = 1 << 20
VMEM = pl.BlockSpec(memory_space=pltpu.VMEM)
SMEM = pl.BlockSpec(memory_space=pltpu.SMEM)


def request_of(slot_ref, slot, lead):
    found = jnp.int32(0)
    for r in lead:
        found = jnp.where(slot_ref[r] == slot, jnp.int32(r), found)
    return found


def norm_kernel(hidden_ref, own_ref, other_ref):
    half = own_ref.shape[1]
    at_depth = lax.axis_index("depth")
    widened = hidden_ref[...].astype(jnp.float32)
    mean_square = jnp.mean(widened * widened, axis=-1, keepdims=True)
    normed = widened * lax.rsqrt(mean_square + 1e-06)
    low, high = normed[:, :half], normed[:, half:]
    first = at_depth == 0
    own_ref[...] = jnp.where(first, low, high).astype(jnp.bfloat16)
    other_ref[...] = jnp.where(first, high, low).astype(jnp.bfloat16)


def query_kernel(sizes, slot_ref, *refs):
    wide, halves, rows = sizes
    pieces = len(refs) - 1 - 4 - 2
    piece_refs, weight_ref = refs[:pieces], refs[pieces]
    out_refs = refs[pieces + 1 : pieces + 5]
    rows_ref, sums_ref = refs[pieces + 5 :]
    at_wide, at_depth = lax.axis_index("wide"), lax.axis_index("depth")
    for k, piece in enumerate(piece_refs):
        rows_ref[k * rows : (k + 1) * rows, :] = piece[...].astype(jnp.float32)
    sums_ref[...] = jnp.dot(
        rows_ref[...].astype(jnp.bfloat16), weight_ref[...], preferred_element_type=jnp.float32
    )
    total = wide * halves * rows
    for k, out in enumerate(out_refs):
        flip_wide, flip_depth = k // 2, k % 2
        peer_wide, peer_depth = at_wide ^ flip_wide, at_depth ^ flip_depth
        for j in range(rows):
            slot = (peer_wide * halves + peer_depth) * rows + j
            r = request_of(slot_ref, slot, range(total))
            from_wide = r // (rows * halves) ^ at_wide
            from_depth = (r // rows) % halves ^ at_depth
            here = (from_wide & 1) == 0
            place = ((from_wide >> 1) * halves + from_depth) * rows + r % rows
            row = sums_ref[pl.ds(place, 1), :]
            out[j : j + 1, :] = jnp.where(here, row, 0.0)


def attend_kernel(sizes, slot_ref, blocks_ref, *refs):
    wide, narrow, halves, rows = sizes
    parts, (keys_ref, values_ref, weight_ref, out_ref) = refs[:4], refs[4:]
    at_wide, at_depth = lax.axis_index("wide"), lax.axis_index("depth")
    cache_len, features = keys_ref.shape[1:]
    heads = features // HDIM
    total = wide * halves * rows
    queries = (parts[0][...] + parts[2][...]) + (parts[1][...] + parts[3][...])
    of_head = (
        lax.broadcasted_iota(jnp.int32, (heads, features), 1) // HDIM
        == lax.broadcasted_iota(jnp.int32, (heads, features), 0)
    )
    positions = lax.broadcasted_iota(jnp.int32, (heads, cache_len), 1)
    contexts = []
    for j in range(rows):
        slot = (at_wide * halves + at_depth) * rows + j
        count = jnp.int32(0)
        for r in range(total):
            count = jnp.where(slot_ref[r] == slot, blocks_ref[r], count)
        spread = jnp.where(of_head, queries[j : j + 1, :], 0.0).astype(jnp.bfloat16)
        scores = lax.dot_general(
            spread, keys_ref[j], (((1,), (1,)), ((), ())), preferred_element_type=jnp.float32
        )
        scores = jnp.where(positions < count * BLOCK, scores, jnp.float32(-1e30))
        row_top = jnp.max(scores, axis=-1, keepdims=True)
        raised = jnp.exp(scores - row_top)
        shares = (raised / jnp.sum(raised, axis=-1, keepdims=True)).astype(jnp.bfloat16)
        mixed = jnp.dot(shares, values_ref[j], preferred_element_type=jnp.float32)
        contexts.append(jnp.sum(jnp.where(of_head, mixed, 0.0), axis=0, keepdims=True))
    padding = jnp.zeros((8 - rows, features), jnp.float32)
    context = jnp.concatenate(contexts + [padding], axis=0).astype(jnp.bfloat16)
    partial = jnp.dot(context, weight_ref[...], preferred_element_type=jnp.float32)
    width = partial.shape[1] // narrow
    for to_wide in range(wide):
        lines = []
        for i in range(rows):
            at = slot_ref[(to_wide * halves + at_depth) * rows + i] - (
                at_wide * halves + at_depth
            ) * rows
            line = jnp.zeros_like(partial[:1])
            for j in range(rows):
                line = jnp.where(at == j, partial[j : j + 1], line)
            lines.append(line)
        block = jnp.concatenate(lines, axis=0).astype(jnp.bfloat16)
        for to_narrow in range(narrow):
            out_ref[to_wide * narrow + to_narrow] = block[
                :, to_narrow * width : (to_narrow + 1) * width
            ]


def sum_kernel(parts_ref, out_ref):
    total = parts_ref[0].astype(jnp.float32)
    for k in range(1, parts_ref.shape[0]):
        total = total + parts_ref[k].astype(jnp.float32)
    out_ref[...] = total.astype(jnp.bfloat16)


def shards(
    hidden_state, query_weight, output_weight, cache_keys, cache_values, enc_blocks, cache_slot
):
    rows = hidden_state.shape[0]
    wide, narrow, halves = (lax.axis_size(name) for name in ("wide", "narrow", "depth"))
    half, features = query_weight.shape
    width = output_weight.shape[1]

    def flipped(x, flip_wide, flip_depth):
        pairs = [
            (w * halves + d, (w ^ flip_wide) * halves + (d ^ flip_depth))
            for w in range(wide)
            for d in range(halves)
        ]
        return lax.ppermute(x, ("wide", "depth"), pairs)

    half_rows = jax.ShapeDtypeStruct((rows, half), jnp.bfloat16)
    own, other = pl.pallas_call(
        norm_kernel,
        out_shape=[half_rows, half_rows],
        in_specs=[VMEM],
        out_specs=[VMEM, VMEM],
        compiler_params=pltpu.CompilerParams(vmem_limit_bytes=MIB),
    )(hidden_state)
    pieces = []
    for chip in range(wide // 2):
        for flip_depth in range(halves):
            if chip == 0 and flip_depth == 0:
                pieces.append(own)
            else:
                pieces.append(flipped(other if flip_depth else own, chip * 2, flip_depth))
    count = len(pieces) * rows
    sums = jax.ShapeDtypeStruct((rows, features), jnp.float32)
    parts = pl.pallas_call(
        lambda *refs: query_kernel((wide, halves, rows), *refs),
        out_shape=[sums] * 4,
        in_specs=[SMEM] + [VMEM] * (len(pieces) + 1),
        out_specs=[VMEM] * 4,
        scratch_shapes=[
            pltpu.VMEM((count, half), jnp.float32),
            pltpu.VMEM((count, features), jnp.float32),
        ],
        compiler_params=pltpu.CompilerParams(vmem_limit_bytes=6 * MIB),
    )(cache_slot, *pieces, query_weight)
    arrived = [parts[0]] + [flipped(parts[k], k // 2, k % 2) for k in range(1, 4)]
    spread = pl.pallas_call(
        lambda *refs: attend_kernel((wide, narrow, halves, rows), *refs),
        out_shape=jax.ShapeDtypeStruct((wide * narrow, rows, width // narrow), jnp.bfloat16),
        in_specs=[SMEM, SMEM] + [VMEM] * 7,
        out_specs=VMEM,
        compiler_params=pltpu.CompilerParams(vmem_limit_bytes=16 * MIB),
    )(cache_slot, enc_blocks, *arrived, cache_keys, cache_values, output_weight)
    gathered = lax.all_to_all(spread, ("wide", "narrow"), 0, 0, tiled=True)
    return pl.pallas_call(
        sum_kernel,
        out_shape=jax.ShapeDtypeStruct((rows, width // narrow), jnp.bfloat16),
        in_specs=[VMEM],
        out_specs=VMEM,
        compiler_params=pltpu.CompilerParams(vmem_limit_bytes=MIB),
    )(gathered)


def solution(mesh):
    placed = (
        P(("wide", "depth"), None),
        P("depth", "narrow"),
        P("narrow", None),
        P(("wide", "depth"), None, "narrow"),
        P(("wide", "depth"), None, "narrow"),
        P(),
        P(),
    )
    return jax.shard_map(
        shards,
        mesh=mesh,
        in_specs=placed,
        out_specs=P(("wide", "depth"), "narrow"),
        check_vma=False,
    )
```

```python
import jax
import jax.numpy as jnp
from jax import lax
from jax.experimental import pallas as pl
from jax.experimental.pallas import tpu as pltpu
from jax.sharding import PartitionSpec as P

HDIM = 64
BLOCK = 128

MIB = 1 << 20
VMEM = pl.BlockSpec(memory_space=pltpu.VMEM)
SMEM = pl.BlockSpec(memory_space=pltpu.SMEM)


def request_of(slot_ref, slot, lead):
    found = jnp.int32(0)
    for r in lead:
        found = jnp.where(slot_ref[r] == slot, jnp.int32(r), found)
    return found


def norm_kernel(hidden_ref, own_ref, other_ref):
    half = own_ref.shape[1]
    at_depth = lax.axis_index("depth")
    widened = hidden_ref[...].astype(jnp.float32)
    mean_square = jnp.mean(widened * widened, axis=-1, keepdims=True)
    normed = widened * lax.rsqrt(mean_square + 1e-06)
    low, high = normed[:, :half], normed[:, half:]
    first = at_depth == 0
    own_ref[...] = jnp.where(first, low, high).astype(jnp.bfloat16)
    other_ref[...] = jnp.where(first, high, low).astype(jnp.bfloat16)


def query_kernel(sizes, slot_ref, *refs):
    wide, halves, rows = sizes
    pieces = len(refs) - 1 - 4 - 2
    piece_refs, weight_ref = refs[:pieces], refs[pieces]
    out_refs = refs[pieces + 1 : pieces + 5]
    rows_ref, sums_ref = refs[pieces + 5 :]
    at_wide, at_depth = lax.axis_index("wide"), lax.axis_index("depth")
    for k, piece in enumerate(piece_refs):
        rows_ref[k * rows : (k + 1) * rows, :] = piece[...].astype(jnp.float32)
    sums_ref[...] = jnp.dot(
        rows_ref[...].astype(jnp.bfloat16), weight_ref[...], preferred_element_type=jnp.float32
    )
    total = wide * halves * rows
    for k, out in enumerate(out_refs):
        flip_wide, flip_depth = k // 2, k % 2
        peer_wide, peer_depth = at_wide ^ flip_wide, at_depth ^ flip_depth
        for j in range(rows):
            slot = (peer_wide * halves + peer_depth) * rows + j
            r = request_of(slot_ref, slot, range(total))
            from_wide = r // (rows * halves) ^ at_wide
            from_depth = (r // rows) % halves ^ at_depth
            here = (from_wide & 1) == 0
            place = ((from_wide >> 1) * halves + from_depth) * rows + r % rows
            row = sums_ref[pl.ds(place, 1), :]
            out[j : j + 1, :] = jnp.where(here, row, 0.0)


def attend_kernel(sizes, slot_ref, blocks_ref, *refs):
    wide, narrow, halves, rows = sizes
    parts, (keys_ref, values_ref, weight_ref, out_ref) = refs[:4], refs[4:]
    at_wide, at_depth = lax.axis_index("wide"), lax.axis_index("depth")
    cache_len, features = keys_ref.shape[1:]
    heads = features // HDIM
    total = wide * halves * rows
    queries = (parts[0][...] + parts[2][...]) + (parts[1][...] + parts[3][...])
    of_head = (
        lax.broadcasted_iota(jnp.int32, (heads, features), 1) // HDIM
        == lax.broadcasted_iota(jnp.int32, (heads, features), 0)
    )
    positions = lax.broadcasted_iota(jnp.int32, (heads, cache_len), 1)
    contexts = []
    for j in range(rows):
        slot = (at_wide * halves + at_depth) * rows + j
        count = jnp.int32(0)
        for r in range(total):
            count = jnp.where(slot_ref[r] == slot, blocks_ref[r], count)
        spread = jnp.where(of_head, queries[j : j + 1, :], 0.0).astype(jnp.bfloat16)
        scores = lax.dot_general(
            spread, keys_ref[j], (((1,), (1,)), ((), ())), preferred_element_type=jnp.float32
        )
        scores = jnp.where(positions < count * BLOCK, scores, jnp.float32(-1e30))
        row_top = jnp.max(scores, axis=-1, keepdims=True)
        raised = jnp.exp(scores - row_top)
        shares = (raised / jnp.sum(raised, axis=-1, keepdims=True)).astype(jnp.bfloat16)
        mixed = jnp.dot(shares, values_ref[j], preferred_element_type=jnp.float32)
        contexts.append(jnp.sum(jnp.where(of_head, mixed, 0.0), axis=0, keepdims=True))
    padding = jnp.zeros((8 - rows, features), jnp.float32)
    context = jnp.concatenate(contexts + [padding], axis=0).astype(jnp.bfloat16)
    partial = jnp.dot(context, weight_ref[...], preferred_element_type=jnp.float32)
    width = partial.shape[1] // narrow
    for to_wide in range(wide):
        lines = []
        for i in range(rows):
            at = slot_ref[(to_wide * halves + at_depth) * rows + i] - (
                at_wide * halves + at_depth
            ) * rows
            line = jnp.zeros_like(partial[:1])
            for j in range(rows):
                line = jnp.where(at == j, partial[j : j + 1], line)
            lines.append(line)
        block = jnp.concatenate(lines, axis=0).astype(jnp.bfloat16)
        for to_narrow in range(narrow):
            out_ref[to_wide * narrow + to_narrow] = block[
                :, to_narrow * width : (to_narrow + 1) * width
            ]


def sum_kernel(parts_ref, out_ref):
    total = parts_ref[0].astype(jnp.float32)
    for k in range(1, parts_ref.shape[0]):
        total = total + parts_ref[k].astype(jnp.float32)
    out_ref[...] = total.astype(jnp.bfloat16)


def shards(
    hidden_state, query_weight, output_weight, cache_keys, cache_values, enc_blocks, cache_slot
):
    rows = hidden_state.shape[0]
    wide, narrow, halves = (lax.axis_size(name) for name in ("wide", "narrow", "depth"))
    half, features = query_weight.shape
    width = output_weight.shape[1]

    def flipped(x, flip_wide, flip_depth):
        pairs = [
            (w * halves + d, (w ^ flip_wide) * halves + (d ^ flip_depth))
            for w in range(wide)
            for d in range(halves)
        ]
        return lax.ppermute(x, ("wide", "depth"), pairs)

    half_rows = jax.ShapeDtypeStruct((rows, half), jnp.bfloat16)
    own, other = pl.pallas_call(
        norm_kernel,
        out_shape=[half_rows, half_rows],
        in_specs=[VMEM],
        out_specs=[VMEM, VMEM],
        compiler_params=pltpu.CompilerParams(vmem_limit_bytes=MIB),
        cost_estimate=pl.CostEstimate(flops=10**10, bytes_accessed=0, transcendentals=0),
    )(hidden_state)
    pieces = []
    for chip in range(wide // 2):
        for flip_depth in range(halves):
            if chip == 0 and flip_depth == 0:
                pieces.append(own)
            else:
                pieces.append(flipped(other if flip_depth else own, chip * 2, flip_depth))
    count = len(pieces) * rows
    sums = jax.ShapeDtypeStruct((rows, features), jnp.float32)
    parts = pl.pallas_call(
        lambda *refs: query_kernel((wide, halves, rows), *refs),
        out_shape=[sums] * 4,
        in_specs=[SMEM] + [VMEM] * (len(pieces) + 1),
        out_specs=[VMEM] * 4,
        scratch_shapes=[
            pltpu.VMEM((count, half), jnp.float32),
            pltpu.VMEM((count, features), jnp.float32),
        ],
        compiler_params=pltpu.CompilerParams(vmem_limit_bytes=6 * MIB),
    )(cache_slot, *pieces, query_weight)
    arrived = [parts[0]] + [flipped(parts[k], k // 2, k % 2) for k in range(1, 4)]
    spread = pl.pallas_call(
        lambda *refs: attend_kernel((wide, narrow, halves, rows), *refs),
        out_shape=jax.ShapeDtypeStruct((wide * narrow, rows, width // narrow), jnp.bfloat16),
        in_specs=[SMEM, SMEM] + [VMEM] * 7,
        out_specs=VMEM,
        compiler_params=pltpu.CompilerParams(vmem_limit_bytes=16 * MIB),
    )(cache_slot, enc_blocks, *arrived, cache_keys, cache_values, output_weight)
    gathered = lax.all_to_all(spread, ("wide", "narrow"), 0, 0, tiled=True)
    return pl.pallas_call(
        sum_kernel,
        out_shape=jax.ShapeDtypeStruct((rows, width // narrow), jnp.bfloat16),
        in_specs=[VMEM],
        out_specs=VMEM,
        compiler_params=pltpu.CompilerParams(vmem_limit_bytes=MIB),
    )(gathered)


def solution(mesh):
    placed = (
        P(("wide", "depth"), None),
        P("depth", "narrow"),
        P("narrow", None),
        P(("wide", "depth"), None, "narrow"),
        P(("wide", "depth"), None, "narrow"),
        P(),
        P(),
    )
    return jax.shard_map(
        shards,
        mesh=mesh,
        in_specs=placed,
        out_specs=P(("wide", "depth"), "narrow"),
        check_vma=False,
    )
```

```python
import jax
import jax.numpy as jnp
from jax import lax
from jax.experimental import pallas as pl
from jax.experimental.pallas import tpu as pltpu
from jax.sharding import PartitionSpec as P

HDIM = 64
BLOCK = 128

MIB = 1 << 20
VMEM = pl.BlockSpec(memory_space=pltpu.VMEM)
SMEM = pl.BlockSpec(memory_space=pltpu.SMEM)


def request_of(slot_ref, slot, lead):
    found = jnp.int32(0)
    for r in lead:
        found = jnp.where(slot_ref[r] == slot, jnp.int32(r), found)
    return found


def crossing(chip, flip_depth):
    return (chip & 1) ^ flip_depth


def norm_kernel(hidden_ref, own_ref, other_ref):
    half = own_ref.shape[1]
    at_depth = lax.axis_index("depth")
    widened = hidden_ref[...].astype(jnp.float32)
    mean_square = jnp.mean(widened * widened, axis=-1, keepdims=True)
    normed = widened * lax.rsqrt(mean_square + 1e-06)
    low, high = normed[:, :half], normed[:, half:]
    first = at_depth == 0
    own_ref[...] = jnp.where(first, low, high).astype(jnp.bfloat16)
    other_ref[...] = jnp.where(first, high, low).astype(jnp.bfloat16)


def query_kernel(sizes, slot_ref, *refs):
    wide, halves, rows = sizes
    pieces = len(refs) - 1 - 4 - 2
    piece_refs, weight_ref = refs[:pieces], refs[pieces]
    out_refs = refs[pieces + 1 : pieces + 5]
    rows_ref, sums_ref = refs[pieces + 5 :]
    at_wide, at_depth = lax.axis_index("wide"), lax.axis_index("depth")
    for k, piece in enumerate(piece_refs):
        rows_ref[k * rows : (k + 1) * rows, :] = piece[...].astype(jnp.float32)
    sums_ref[...] = jnp.dot(
        rows_ref[...].astype(jnp.bfloat16), weight_ref[...], preferred_element_type=jnp.float32
    )
    total = wide * halves * rows
    for k, out in enumerate(out_refs):
        flip_wide, flip_depth = k // 2, k % 2
        peer_wide, peer_depth = at_wide ^ flip_wide, at_depth ^ flip_depth
        for j in range(rows):
            slot = (peer_wide * halves + peer_depth) * rows + j
            r = request_of(slot_ref, slot, range(total))
            from_wide = r // (rows * halves) ^ at_wide
            from_depth = (r // rows) % halves ^ at_depth
            here = (from_wide & 1) == crossing(from_wide >> 1, from_depth)
            place = ((from_wide >> 1) * halves + from_depth) * rows + r % rows
            row = sums_ref[pl.ds(place, 1), :]
            out[j : j + 1, :] = jnp.where(here, row, 0.0)


def attend_kernel(sizes, slot_ref, blocks_ref, *refs):
    wide, narrow, halves, rows = sizes
    parts, (keys_ref, values_ref, weight_ref, out_ref) = refs[:4], refs[4:]
    at_wide, at_depth = lax.axis_index("wide"), lax.axis_index("depth")
    cache_len, features = keys_ref.shape[1:]
    heads = features // HDIM
    total = wide * halves * rows
    queries = (parts[0][...] + parts[2][...]) + (parts[1][...] + parts[3][...])
    of_head = (
        lax.broadcasted_iota(jnp.int32, (heads, features), 1) // HDIM
        == lax.broadcasted_iota(jnp.int32, (heads, features), 0)
    )
    positions = lax.broadcasted_iota(jnp.int32, (heads, cache_len), 1)
    contexts = []
    for j in range(rows):
        slot = (at_wide * halves + at_depth) * rows + j
        count = jnp.int32(0)
        for r in range(total):
            count = jnp.where(slot_ref[r] == slot, blocks_ref[r], count)
        spread = jnp.where(of_head, queries[j : j + 1, :], 0.0).astype(jnp.bfloat16)
        scores = lax.dot_general(
            spread, keys_ref[j], (((1,), (1,)), ((), ())), preferred_element_type=jnp.float32
        )
        scores = jnp.where(positions < count * BLOCK, scores, jnp.float32(-1e30))
        row_top = jnp.max(scores, axis=-1, keepdims=True)
        raised = jnp.exp(scores - row_top)
        shares = (raised / jnp.sum(raised, axis=-1, keepdims=True)).astype(jnp.bfloat16)
        mixed = jnp.dot(shares, values_ref[j], preferred_element_type=jnp.float32)
        contexts.append(jnp.sum(jnp.where(of_head, mixed, 0.0), axis=0, keepdims=True))
    padding = jnp.zeros((8 - rows, features), jnp.float32)
    context = jnp.concatenate(contexts + [padding], axis=0).astype(jnp.bfloat16)
    partial = jnp.dot(context, weight_ref[...], preferred_element_type=jnp.float32)
    width = partial.shape[1] // narrow
    for to_wide in range(wide):
        lines = []
        for i in range(rows):
            at = slot_ref[(to_wide * halves + at_depth) * rows + i] - (
                at_wide * halves + at_depth
            ) * rows
            line = jnp.zeros_like(partial[:1])
            for j in range(rows):
                line = jnp.where(at == j, partial[j : j + 1], line)
            lines.append(line)
        block = jnp.concatenate(lines, axis=0).astype(jnp.bfloat16)
        for to_narrow in range(narrow):
            out_ref[to_wide * narrow + to_narrow] = block[
                :, to_narrow * width : (to_narrow + 1) * width
            ]


def sum_kernel(parts_ref, out_ref):
    total = parts_ref[0].astype(jnp.float32)
    for k in range(1, parts_ref.shape[0]):
        total = total + parts_ref[k].astype(jnp.float32)
    out_ref[...] = total.astype(jnp.bfloat16)


def shards(
    hidden_state, query_weight, output_weight, cache_keys, cache_values, enc_blocks, cache_slot
):
    rows = hidden_state.shape[0]
    wide, narrow, halves = (lax.axis_size(name) for name in ("wide", "narrow", "depth"))
    half, features = query_weight.shape
    width = output_weight.shape[1]

    def flipped(x, flip_wide, flip_depth):
        pairs = [
            (w * halves + d, (w ^ flip_wide) * halves + (d ^ flip_depth))
            for w in range(wide)
            for d in range(halves)
        ]
        return lax.ppermute(x, ("wide", "depth"), pairs)

    half_rows = jax.ShapeDtypeStruct((rows, half), jnp.bfloat16)
    own, other = pl.pallas_call(
        norm_kernel,
        out_shape=[half_rows, half_rows],
        in_specs=[VMEM],
        out_specs=[VMEM, VMEM],
        compiler_params=pltpu.CompilerParams(vmem_limit_bytes=MIB),
        cost_estimate=pl.CostEstimate(flops=10**10, bytes_accessed=0, transcendentals=0),
    )(hidden_state)
    pieces = []
    for chip in range(wide // 2):
        for flip_depth in range(halves):
            if chip == 0 and flip_depth == 0:
                pieces.append(own)
            else:
                flip_wide = chip * 2 + crossing(chip, flip_depth)
                pieces.append(flipped(other if flip_depth else own, flip_wide, flip_depth))
    count = len(pieces) * rows
    sums = jax.ShapeDtypeStruct((rows, features), jnp.float32)
    parts = pl.pallas_call(
        lambda *refs: query_kernel((wide, halves, rows), *refs),
        out_shape=[sums] * 4,
        in_specs=[SMEM] + [VMEM] * (len(pieces) + 1),
        out_specs=[VMEM] * 4,
        scratch_shapes=[
            pltpu.VMEM((count, half), jnp.float32),
            pltpu.VMEM((count, features), jnp.float32),
        ],
        compiler_params=pltpu.CompilerParams(vmem_limit_bytes=6 * MIB),
    )(cache_slot, *pieces, query_weight)
    arrived = [parts[0]] + [flipped(parts[k], k // 2, k % 2) for k in range(1, 4)]
    spread = pl.pallas_call(
        lambda *refs: attend_kernel((wide, narrow, halves, rows), *refs),
        out_shape=jax.ShapeDtypeStruct((wide * narrow, rows, width // narrow), jnp.bfloat16),
        in_specs=[SMEM, SMEM] + [VMEM] * 7,
        out_specs=VMEM,
        compiler_params=pltpu.CompilerParams(vmem_limit_bytes=16 * MIB),
    )(cache_slot, enc_blocks, *arrived, cache_keys, cache_values, output_weight)
    gathered = lax.all_to_all(spread, ("wide", "narrow"), 0, 0, tiled=True)
    return pl.pallas_call(
        sum_kernel,
        out_shape=jax.ShapeDtypeStruct((rows, width // narrow), jnp.bfloat16),
        in_specs=[VMEM],
        out_specs=VMEM,
        compiler_params=pltpu.CompilerParams(vmem_limit_bytes=MIB),
    )(gathered)


def solution(mesh):
    placed = (
        P(("wide", "depth"), None),
        P("depth", "narrow"),
        P("narrow", None),
        P(("wide", "depth"), None, "narrow"),
        P(("wide", "depth"), None, "narrow"),
        P(),
        P(),
    )
    return jax.shard_map(
        shards,
        mesh=mesh,
        in_specs=placed,
        out_specs=P(("wide", "depth"), "narrow"),
        check_vma=False,
    )
```

```python
import jax
import jax.numpy as jnp
from jax import lax
from jax.experimental import pallas as pl
from jax.experimental.pallas import tpu as pltpu
from jax.sharding import PartitionSpec as P

HDIM = 64
BLOCK = 128
SUBLANES = 8
LANES = 128

MIB = 1 << 20
VMEM = pl.BlockSpec(memory_space=pltpu.VMEM)


def crossing(chip, flip_depth):
    return (chip & 1) ^ flip_depth


def table_kernel(sizes, slot_ref, blocks_ref, place_ref, limit_ref, route_ref):
    wide, halves, rows = sizes
    at_wide, at_depth = lax.axis_index("wide"), lax.axis_index("depth")
    total = slot_ref.shape[1]
    slots = slot_ref[...]

    def iota(count, dim):
        return lax.broadcasted_iota(jnp.int32, (count, total), dim)

    target = iota(SUBLANES, 0)
    peer = target // rows
    slot = ((at_wide ^ (peer // 2)) * halves + (at_depth ^ (peer % 2))) * rows + target % rows
    request = jnp.sum(jnp.where(slots == slot, iota(SUBLANES, 1), 0), axis=1, keepdims=True)
    from_wide = (request // (rows * halves)) ^ at_wide
    from_depth = (request // rows % halves) ^ at_depth
    place = ((from_wide >> 1) * halves + from_depth) * rows + request % rows
    here = (from_wide & 1) == crossing(from_wide >> 1, from_depth)
    place_ref[...] = jnp.broadcast_to(jnp.where(here, place, -1), place_ref.shape)
    base = (at_wide * halves + at_depth) * rows
    for j in range(rows):
        count = jnp.sum(jnp.where(slots == base + j, blocks_ref[...], 0), axis=1, keepdims=True)
        limit_ref[j] = jnp.broadcast_to(count * BLOCK, limit_ref.shape[1:])
    line = iota(wide * rows, 0)
    request = (line // rows * halves + at_depth) * rows + line % rows
    held = jnp.sum(jnp.where(iota(wide * rows, 1) == request, slots, 0), axis=1, keepdims=True)
    route_ref[...] = jnp.broadcast_to(held - base, route_ref.shape)


def query_kernel(rows, place_ref, *refs):
    pieces = len(refs) - 1 - 4 - 1
    piece_refs, weight_ref = refs[:pieces], refs[pieces]
    out_refs, rows_ref = refs[pieces + 1 : pieces + 5], refs[pieces + 5]
    half = weight_ref.shape[0]
    at_depth = lax.axis_index("depth")
    for k, piece in enumerate(piece_refs):
        rows_ref[k * rows : (k + 1) * rows, :] = piece[...].astype(jnp.float32)
    widened = rows_ref[...]
    mean_square = jnp.mean(widened * widened, axis=-1, keepdims=True)
    used = rows_ref[:, pl.ds(pl.multiple_of(at_depth * half, LANES), half)]
    normed = (used * lax.rsqrt(mean_square + 1e-06)).astype(jnp.bfloat16)
    sums = jnp.dot(normed, weight_ref[...], preferred_element_type=jnp.float32)
    place = place_ref[...]
    for c in range(sums.shape[1] // LANES):
        span = slice(c * LANES, (c + 1) * LANES)
        picked = jnp.zeros_like(place, jnp.float32)
        for g in range(sums.shape[0] // SUBLANES):
            lines = sums[g * SUBLANES : (g + 1) * SUBLANES, span]
            found = jnp.take_along_axis(lines, place & (SUBLANES - 1), axis=0)
            picked = jnp.where(place >> 3 == g, found, picked)
        for k, out in enumerate(out_refs):
            out[:, span] = picked[k * rows : (k + 1) * rows]


def attend_kernel(narrow, limit_ref, route_ref, *refs):
    parts, (keys_ref, values_ref, weight_ref, out_ref) = refs[:4], refs[4:]
    rows, cache_len, features = keys_ref.shape
    heads = features // HDIM
    queries = (parts[0][...] + parts[2][...]) + (parts[1][...] + parts[3][...])
    of_head = (
        lax.broadcasted_iota(jnp.int32, (heads, features), 1) // HDIM
        == lax.broadcasted_iota(jnp.int32, (heads, features), 0)
    )
    positions = lax.broadcasted_iota(jnp.int32, (heads, cache_len), 1)
    scores, shares, mixed = [], [], []
    for j in range(rows):
        spread = jnp.where(of_head, queries[j : j + 1, :], 0.0).astype(jnp.bfloat16)
        scores.append(
            lax.dot_general(
                spread, keys_ref[j], (((1,), (1,)), ((), ())), preferred_element_type=jnp.float32
            )
        )
    for j in range(rows):
        masked = jnp.where(positions < limit_ref[j], scores[j], jnp.float32(-1e30))
        row_top = jnp.max(masked, axis=-1, keepdims=True)
        raised = jnp.exp(masked - row_top)
        shares.append((raised / jnp.sum(raised, axis=-1, keepdims=True)).astype(jnp.bfloat16))
    for j in range(rows):
        mixed.append(jnp.dot(shares[j], values_ref[j], preferred_element_type=jnp.float32))
    route = route_ref[...]
    context = jnp.zeros(route.shape, jnp.float32)
    for j in range(rows):
        line = jnp.sum(jnp.where(of_head, mixed[j], 0.0), axis=0, keepdims=True)
        context = jnp.where(route == j, line, context)
    partial = jnp.dot(
        context.astype(jnp.bfloat16), weight_ref[...], preferred_element_type=jnp.float32
    )
    width = partial.shape[1] // narrow
    for to_wide in range(partial.shape[0] // rows):
        block = partial[to_wide * rows : (to_wide + 1) * rows].astype(jnp.bfloat16)
        for to_narrow in range(narrow):
            out_ref[to_wide * narrow + to_narrow] = block[
                :, to_narrow * width : (to_narrow + 1) * width
            ]


def sum_kernel(parts_ref, out_ref):
    total = parts_ref[0].astype(jnp.float32)
    for k in range(1, parts_ref.shape[0]):
        total = total + parts_ref[k].astype(jnp.float32)
    out_ref[...] = total.astype(jnp.bfloat16)


def local_call(kernel, out_shape, count, mib, scratch=(), cost=None):
    several = isinstance(out_shape, list)
    return pl.pallas_call(
        kernel,
        out_shape=out_shape,
        in_specs=[VMEM] * count,
        out_specs=[VMEM] * len(out_shape) if several else VMEM,
        scratch_shapes=scratch,
        compiler_params=pltpu.CompilerParams(vmem_limit_bytes=mib * MIB),
        cost_estimate=cost,
    )


def shards(
    hidden_state, query_weight, output_weight, cache_keys, cache_values, enc_blocks, cache_slot
):
    rows, model = hidden_state.shape
    wide, narrow, halves = (lax.axis_size(name) for name in ("wide", "narrow", "depth"))
    features = query_weight.shape[1]
    cache_len = cache_keys.shape[1]
    width = output_weight.shape[1]

    def flipped(x, flip_wide, flip_depth):
        pairs = [
            (w * halves + d, (w ^ flip_wide) * halves + (d ^ flip_depth))
            for w in range(wide)
            for d in range(halves)
        ]
        return lax.ppermute(x, ("wide", "depth"), pairs)

    shape = jax.ShapeDtypeStruct
    place, limit, route = local_call(
        lambda *refs: table_kernel((wide, halves, rows), *refs),
        [
            shape((4 * rows, LANES), jnp.int32),
            shape((rows, features // HDIM, cache_len), jnp.int32),
            shape((wide * rows, features), jnp.int32),
        ],
        2,
        1,
        cost=pl.CostEstimate(flops=10**10, bytes_accessed=0, transcendentals=0),
    )(cache_slot[None], enc_blocks[None])
    pieces = []
    for chip in range(wide // 2):
        for flip_depth in range(halves):
            if chip == 0 and flip_depth == 0:
                pieces.append(hidden_state)
            else:
                flip_wide = chip * 2 + crossing(chip, flip_depth)
                pieces.append(flipped(hidden_state, flip_wide, flip_depth))
    parts = local_call(
        lambda *refs: query_kernel(rows, *refs),
        [shape((rows, features), jnp.float32)] * 4,
        len(pieces) + 2,
        6,
        scratch=[pltpu.VMEM((len(pieces) * rows, model), jnp.float32)],
    )(place, *pieces, query_weight)
    arrived = [parts[0]] + [flipped(parts[k], k // 2, k % 2) for k in range(1, 4)]
    spread = local_call(
        lambda *refs: attend_kernel(narrow, *refs),
        shape((wide * narrow, rows, width // narrow), jnp.bfloat16),
        9,
        16,
    )(limit, route, *arrived, cache_keys, cache_values, output_weight)
    gathered = lax.all_to_all(spread, ("wide", "narrow"), 0, 0, tiled=True)
    return local_call(
        sum_kernel, shape((rows, width // narrow), jnp.bfloat16), 1, 1
    )(gathered)


def solution(mesh):
    placed = (
        P(("wide", "depth"), None),
        P("depth", "narrow"),
        P("narrow", None),
        P(("wide", "depth"), None, "narrow"),
        P(("wide", "depth"), None, "narrow"),
        P(),
        P(),
    )
    return jax.shard_map(
        shards,
        mesh=mesh,
        in_specs=placed,
        out_specs=P(("wide", "depth"), "narrow"),
        check_vma=False,
    )
```

```python
import jax
import jax.numpy as jnp
from jax import lax
from jax.experimental import pallas as pl
from jax.experimental.pallas import tpu as pltpu
from jax.sharding import PartitionSpec as P

HDIM = 64
BLOCK = 128
SUBLANES = 8
LANES = 128

MIB = 1 << 20
VMEM = pl.BlockSpec(memory_space=pltpu.VMEM)


def crossing(chip, flip_depth):
    return (chip & 1) ^ flip_depth


def norm_kernel(hidden_ref, own_ref, other_ref):
    half = own_ref.shape[1]
    at_depth = lax.axis_index("depth")
    widened = hidden_ref[...].astype(jnp.float32)
    mean_square = jnp.mean(widened * widened, axis=-1, keepdims=True)
    normed = widened * lax.rsqrt(mean_square + 1e-06)
    low, high = normed[:, :half], normed[:, half:]
    first = at_depth == 0
    own_ref[...] = jnp.where(first, low, high).astype(jnp.bfloat16)
    other_ref[...] = jnp.where(first, high, low).astype(jnp.bfloat16)


def table_kernel(sizes, slot_hbm, blocks_hbm, place_ref, limit_ref, route_ref, *scratch):
    wide, halves, rows = sizes
    slot_ref, blocks_ref, slot_sem, blocks_sem = scratch
    slot_copy = pltpu.make_async_copy(slot_hbm, slot_ref, slot_sem)
    blocks_copy = pltpu.make_async_copy(blocks_hbm, blocks_ref, blocks_sem)
    slot_copy.start()
    blocks_copy.start()
    slot_copy.wait()
    blocks_copy.wait()
    at_wide, at_depth = lax.axis_index("wide"), lax.axis_index("depth")
    total = slot_ref.shape[1]
    slots = slot_ref[...]

    def iota(count, dim):
        return lax.broadcasted_iota(jnp.int32, (count, total), dim)

    target = iota(SUBLANES, 0)
    peer = target // rows
    slot = ((at_wide ^ (peer // 2)) * halves + (at_depth ^ (peer % 2))) * rows + target % rows
    request = jnp.sum(jnp.where(slots == slot, iota(SUBLANES, 1), 0), axis=1, keepdims=True)
    from_wide = (request // (rows * halves)) ^ at_wide
    from_depth = (request // rows % halves) ^ at_depth
    place = ((from_wide >> 1) * halves + from_depth) * rows + request % rows
    here = (from_wide & 1) == crossing(from_wide >> 1, from_depth)
    place_ref[...] = jnp.broadcast_to(jnp.where(here, place, -1), place_ref.shape)
    base = (at_wide * halves + at_depth) * rows
    for j in range(rows):
        count = jnp.sum(jnp.where(slots == base + j, blocks_ref[...], 0), axis=1, keepdims=True)
        limit_ref[j] = jnp.broadcast_to(count * BLOCK, limit_ref.shape[1:])
    line = iota(wide * rows, 0)
    request = (line // rows * halves + at_depth) * rows + line % rows
    held = jnp.sum(jnp.where(iota(wide * rows, 1) == request, slots, 0), axis=1, keepdims=True)
    route_ref[...] = jnp.broadcast_to(held - base, route_ref.shape)


def query_kernel(rows, place_ref, *refs):
    pieces = len(refs) - 1 - 4 - 1
    piece_refs, weight_ref = refs[:pieces], refs[pieces]
    out_refs, rows_ref = refs[pieces + 1 : pieces + 5], refs[pieces + 5]
    for k, piece in enumerate(piece_refs):
        rows_ref[k * rows : (k + 1) * rows, :] = piece[...].astype(jnp.float32)
    sums = jnp.dot(
        rows_ref[...].astype(jnp.bfloat16), weight_ref[...], preferred_element_type=jnp.float32
    )
    place = place_ref[...]
    for c in range(sums.shape[1] // LANES):
        span = slice(c * LANES, (c + 1) * LANES)
        picked = jnp.zeros_like(place, jnp.float32)
        for g in range(sums.shape[0] // SUBLANES):
            lines = sums[g * SUBLANES : (g + 1) * SUBLANES, span]
            found = jnp.take_along_axis(lines, place & (SUBLANES - 1), axis=0)
            picked = jnp.where(place >> 3 == g, found, picked)
        for k, out in enumerate(out_refs):
            out[:, span] = picked[k * rows : (k + 1) * rows]


def attend_kernel(narrow, limit_ref, route_ref, *refs):
    parts, (keys_ref, values_ref, weight_ref, out_ref) = refs[:4], refs[4:]
    rows, cache_len, features = keys_ref.shape
    heads = features // HDIM
    queries = (parts[0][...] + parts[2][...]) + (parts[1][...] + parts[3][...])
    of_head = (
        lax.broadcasted_iota(jnp.int32, (heads, features), 1) // HDIM
        == lax.broadcasted_iota(jnp.int32, (heads, features), 0)
    )
    positions = lax.broadcasted_iota(jnp.int32, (heads, cache_len), 1)
    scores, shares, mixed = [], [], []
    for j in range(rows):
        spread = jnp.where(of_head, queries[j : j + 1, :], 0.0).astype(jnp.bfloat16)
        scores.append(
            lax.dot_general(
                spread, keys_ref[j], (((1,), (1,)), ((), ())), preferred_element_type=jnp.float32
            )
        )
    for j in range(rows):
        masked = jnp.where(positions < limit_ref[j], scores[j], jnp.float32(-1e30))
        row_top = jnp.max(masked, axis=-1, keepdims=True)
        raised = jnp.exp(masked - row_top)
        shares.append((raised / jnp.sum(raised, axis=-1, keepdims=True)).astype(jnp.bfloat16))
    for j in range(rows):
        mixed.append(jnp.dot(shares[j], values_ref[j], preferred_element_type=jnp.float32))
    route = route_ref[...]
    context = jnp.zeros(route.shape, jnp.float32)
    for j in range(rows):
        line = jnp.sum(jnp.where(of_head, mixed[j], 0.0), axis=0, keepdims=True)
        context = jnp.where(route == j, line, context)
    partial = jnp.dot(
        context.astype(jnp.bfloat16), weight_ref[...], preferred_element_type=jnp.float32
    )
    width = partial.shape[1] // narrow
    for to_wide in range(partial.shape[0] // rows):
        block = partial[to_wide * rows : (to_wide + 1) * rows].astype(jnp.bfloat16)
        for to_narrow in range(narrow):
            out_ref[to_wide * narrow + to_narrow] = block[
                :, to_narrow * width : (to_narrow + 1) * width
            ]


def sum_kernel(parts_ref, out_ref):
    total = parts_ref[0].astype(jnp.float32)
    for k in range(1, parts_ref.shape[0]):
        total = total + parts_ref[k].astype(jnp.float32)
    out_ref[...] = total.astype(jnp.bfloat16)


def local_call(kernel, out_shape, count, mib, scratch=(), cost=None, spec=VMEM):
    several = isinstance(out_shape, list)
    return pl.pallas_call(
        kernel,
        out_shape=out_shape,
        in_specs=[spec] * count,
        out_specs=[VMEM] * len(out_shape) if several else VMEM,
        scratch_shapes=scratch,
        compiler_params=pltpu.CompilerParams(vmem_limit_bytes=mib * MIB),
        cost_estimate=cost,
    )


def cost_of(flops):
    return pl.CostEstimate(flops=flops, bytes_accessed=0, transcendentals=0)


def shards(
    hidden_state, query_weight, output_weight, cache_keys, cache_values, enc_blocks, cache_slot
):
    rows = hidden_state.shape[0]
    wide, narrow, halves = (lax.axis_size(name) for name in ("wide", "narrow", "depth"))
    features = query_weight.shape[1]
    cache_len = cache_keys.shape[1]
    width = output_weight.shape[1]

    def flipped(x, flip_wide, flip_depth):
        pairs = [
            (w * halves + d, (w ^ flip_wide) * halves + (d ^ flip_depth))
            for w in range(wide)
            for d in range(halves)
        ]
        return lax.ppermute(x, ("wide", "depth"), pairs)

    shape = jax.ShapeDtypeStruct
    place, limit, route = local_call(
        lambda *refs: table_kernel((wide, halves, rows), *refs),
        [
            shape((4 * rows, LANES), jnp.int32),
            shape((rows, features // HDIM, cache_len), jnp.int32),
            shape((wide * rows, features), jnp.int32),
        ],
        2,
        1,
        scratch=[
            pltpu.VMEM((1, cache_slot.shape[0]), jnp.int32),
            pltpu.VMEM((1, cache_slot.shape[0]), jnp.int32),
            pltpu.SemaphoreType.DMA(()),
            pltpu.SemaphoreType.DMA(()),
        ],
        cost=cost_of(10**9),
        spec=pl.BlockSpec(memory_space=pltpu.HBM),
    )(cache_slot[None], enc_blocks[None])
    half_rows = shape((rows, query_weight.shape[0]), jnp.bfloat16)
    own, other = local_call(norm_kernel, [half_rows, half_rows], 1, 1, cost=cost_of(5 * 10**9))(hidden_state)
    pieces = []
    for chip in range(wide // 2):
        for flip_depth in range(halves):
            if chip == 0 and flip_depth == 0:
                pieces.append(own)
            else:
                flip_wide = chip * 2 + crossing(chip, flip_depth)
                pieces.append(flipped(other if flip_depth else own, flip_wide, flip_depth))
    parts = local_call(
        lambda *refs: query_kernel(rows, *refs),
        [shape((rows, features), jnp.float32)] * 4,
        len(pieces) + 2,
        6,
        scratch=[pltpu.VMEM((len(pieces) * rows, query_weight.shape[0]), jnp.float32)],
    )(place, *pieces, query_weight)
    arrived = [parts[0]] + [flipped(parts[k], k // 2, k % 2) for k in range(1, 4)]
    spread = local_call(
        lambda *refs: attend_kernel(narrow, *refs),
        shape((wide * narrow, rows, width // narrow), jnp.bfloat16),
        9,
        16,
    )(limit, route, *arrived, cache_keys, cache_values, output_weight)
    gathered = lax.all_to_all(spread, ("wide", "narrow"), 0, 0, tiled=True)
    return local_call(
        sum_kernel, shape((rows, width // narrow), jnp.bfloat16), 1, 1
    )(gathered)


def solution(mesh):
    placed = (
        P(("wide", "depth"), None),
        P("depth", "narrow"),
        P("narrow", None),
        P(("wide", "depth"), None, "narrow"),
        P(("wide", "depth"), None, "narrow"),
        P(),
        P(),
    )
    return jax.shard_map(
        shards,
        mesh=mesh,
        in_specs=placed,
        out_specs=P(("wide", "depth"), "narrow"),
        check_vma=False,
    )
```

```python
import jax
import jax.numpy as jnp
from jax import lax
from jax.experimental import pallas as pl
from jax.experimental.pallas import tpu as pltpu
from jax.sharding import PartitionSpec as P

HDIM = 64
BLOCK = 128
SUBLANES = 8
LANES = 128

MIB = 1 << 20
VMEM = pl.BlockSpec(memory_space=pltpu.VMEM)


def crossing(chip, flip_depth):
    return (chip & 1) ^ flip_depth


def norm_kernel(hidden_ref, own_ref, other_ref):
    half = own_ref.shape[1]
    at_depth = lax.axis_index("depth")
    widened = hidden_ref[...].astype(jnp.float32)
    mean_square = jnp.mean(widened * widened, axis=-1, keepdims=True)
    normed = widened * lax.rsqrt(mean_square + 1e-06)
    low, high = normed[:, :half], normed[:, half:]
    first = at_depth == 0
    own_ref[...] = jnp.where(first, low, high).astype(jnp.bfloat16)
    other_ref[...] = jnp.where(first, high, low).astype(jnp.bfloat16)


def table_kernel(sizes, slot_hbm, blocks_hbm, place_ref, limit_ref, route_ref, *scratch):
    wide, halves, rows = sizes
    slot_ref, blocks_ref, slot_sem, blocks_sem = scratch
    slot_copy = pltpu.make_async_copy(slot_hbm, slot_ref, slot_sem)
    blocks_copy = pltpu.make_async_copy(blocks_hbm, blocks_ref, blocks_sem)
    slot_copy.start()
    blocks_copy.start()
    slot_copy.wait()
    blocks_copy.wait()
    at_wide, at_depth = lax.axis_index("wide"), lax.axis_index("depth")
    total = slot_ref.shape[1]
    slots = slot_ref[...]

    def iota(count, dim):
        return lax.broadcasted_iota(jnp.int32, (count, total), dim)

    target = iota(SUBLANES, 0)
    peer = target // rows
    slot = ((at_wide ^ (peer // 2)) * halves + (at_depth ^ (peer % 2))) * rows + target % rows
    request = jnp.sum(jnp.where(slots == slot, iota(SUBLANES, 1), 0), axis=1, keepdims=True)
    from_wide = (request // (rows * halves)) ^ at_wide
    from_depth = (request // rows % halves) ^ at_depth
    place = ((from_wide >> 1) * halves + from_depth) * rows + request % rows
    here = (from_wide & 1) == crossing(from_wide >> 1, from_depth)
    place_ref[...] = jnp.broadcast_to(jnp.where(here, place, -1), place_ref.shape)
    base = (at_wide * halves + at_depth) * rows
    for j in range(rows):
        count = jnp.sum(jnp.where(slots == base + j, blocks_ref[...], 0), axis=1, keepdims=True)
        limit_ref[j] = jnp.broadcast_to(count * BLOCK, limit_ref.shape[1:])
    line = iota(wide * rows, 0)
    request = (line // rows * halves + at_depth) * rows + line % rows
    held = jnp.sum(jnp.where(iota(wide * rows, 1) == request, slots, 0), axis=1, keepdims=True)
    route_ref[...] = jnp.broadcast_to(held - base, route_ref.shape)


def query_kernel(rows, order, place_ref, *refs):
    pieces = len(refs) - 1 - 4 - 1
    piece_refs, weight_ref = refs[:pieces], refs[pieces]
    out_refs, rows_ref = refs[pieces + 1 : pieces + 5], refs[pieces + 5]
    for k, piece in zip(order, piece_refs):
        rows_ref[k * rows : (k + 1) * rows, :] = piece[...].astype(jnp.float32)
    sums = jnp.dot(
        rows_ref[...].astype(jnp.bfloat16), weight_ref[...], preferred_element_type=jnp.float32
    )
    place = place_ref[...]
    for c in range(sums.shape[1] // LANES):
        span = slice(c * LANES, (c + 1) * LANES)
        picked = jnp.zeros_like(place, jnp.float32)
        for g in range(sums.shape[0] // SUBLANES):
            lines = sums[g * SUBLANES : (g + 1) * SUBLANES, span]
            found = jnp.take_along_axis(lines, place & (SUBLANES - 1), axis=0)
            picked = jnp.where(place >> 3 == g, found, picked)
        for k, out in enumerate(out_refs):
            out[:, span] = picked[k * rows : (k + 1) * rows]


def attend_kernel(narrow, limit_ref, route_ref, *refs):
    parts, (keys_ref, values_ref, weight_ref, out_ref) = refs[:4], refs[4:]
    rows, cache_len, features = keys_ref.shape
    heads = features // HDIM
    queries = (parts[0][...] + parts[2][...]) + (parts[1][...] + parts[3][...])
    of_head = (
        lax.broadcasted_iota(jnp.int32, (heads, features), 1) // HDIM
        == lax.broadcasted_iota(jnp.int32, (heads, features), 0)
    )
    positions = lax.broadcasted_iota(jnp.int32, (heads, cache_len), 1)
    scores, shares, mixed = [], [], []
    for j in range(rows):
        spread = jnp.where(of_head, queries[j : j + 1, :], 0.0).astype(jnp.bfloat16)
        scores.append(
            lax.dot_general(
                spread, keys_ref[j], (((1,), (1,)), ((), ())), preferred_element_type=jnp.float32
            )
        )
    for j in range(rows):
        masked = jnp.where(positions < limit_ref[j], scores[j], jnp.float32(-1e30))
        row_top = jnp.max(masked, axis=-1, keepdims=True)
        raised = jnp.exp(masked - row_top)
        shares.append((raised / jnp.sum(raised, axis=-1, keepdims=True)).astype(jnp.bfloat16))
    for j in range(rows):
        mixed.append(jnp.dot(shares[j], values_ref[j], preferred_element_type=jnp.float32))
    route = route_ref[...]
    context = jnp.zeros(route.shape, jnp.float32)
    for j in range(rows):
        line = jnp.sum(jnp.where(of_head, mixed[j], 0.0), axis=0, keepdims=True)
        context = jnp.where(route == j, line, context)
    partial = jnp.dot(
        context.astype(jnp.bfloat16), weight_ref[...], preferred_element_type=jnp.float32
    )
    width = partial.shape[1] // narrow
    for to_wide in range(partial.shape[0] // rows):
        block = partial[to_wide * rows : (to_wide + 1) * rows].astype(jnp.bfloat16)
        for to_narrow in range(narrow):
            out_ref[to_wide * narrow + to_narrow] = block[
                :, to_narrow * width : (to_narrow + 1) * width
            ]


def sum_kernel(parts_ref, out_ref):
    total = parts_ref[0].astype(jnp.float32)
    for k in range(1, parts_ref.shape[0]):
        total = total + parts_ref[k].astype(jnp.float32)
    out_ref[...] = total.astype(jnp.bfloat16)


def local_call(kernel, out_shape, count, mib, scratch=(), cost=None, spec=VMEM):
    several = isinstance(out_shape, list)
    return pl.pallas_call(
        kernel,
        out_shape=out_shape,
        in_specs=[spec] * count,
        out_specs=[VMEM] * len(out_shape) if several else VMEM,
        scratch_shapes=scratch,
        compiler_params=pltpu.CompilerParams(vmem_limit_bytes=mib * MIB),
        cost_estimate=cost,
    )


def cost_of(flops):
    return pl.CostEstimate(flops=flops, bytes_accessed=0, transcendentals=0)


def shards(
    hidden_state, query_weight, output_weight, cache_keys, cache_values, enc_blocks, cache_slot
):
    rows = hidden_state.shape[0]
    wide, narrow, halves = (lax.axis_size(name) for name in ("wide", "narrow", "depth"))
    features = query_weight.shape[1]
    cache_len = cache_keys.shape[1]
    width = output_weight.shape[1]

    def flipped(x, flip_wide, flip_depth):
        pairs = [
            (w * halves + d, (w ^ flip_wide) * halves + (d ^ flip_depth))
            for w in range(wide)
            for d in range(halves)
        ]
        return lax.ppermute(x, ("wide", "depth"), pairs)

    shape = jax.ShapeDtypeStruct
    place, limit, route = local_call(
        lambda *refs: table_kernel((wide, halves, rows), *refs),
        [
            shape((4 * rows, LANES), jnp.int32),
            shape((rows, features // HDIM, cache_len), jnp.int32),
            shape((wide * rows, features), jnp.int32),
        ],
        2,
        1,
        scratch=[
            pltpu.VMEM((1, cache_slot.shape[0]), jnp.int32),
            pltpu.VMEM((1, cache_slot.shape[0]), jnp.int32),
            pltpu.SemaphoreType.DMA(()),
            pltpu.SemaphoreType.DMA(()),
        ],
        cost=cost_of(10**9),
        spec=pl.BlockSpec(memory_space=pltpu.HBM),
    )(cache_slot[None], enc_blocks[None])
    half_rows = shape((rows, query_weight.shape[0]), jnp.bfloat16)
    own, other = local_call(norm_kernel, [half_rows, half_rows], 1, 1, cost=cost_of(5 * 10**9))(hidden_state)
    pieces, order = [own], [0]
    for k in range(1, wide // 2 * halves):
        chip, flip_depth = k // halves, k % halves
        flip_wide = chip * 2 + crossing(chip, flip_depth)
        pieces.append(flipped(other if flip_depth else own, flip_wide, flip_depth))
        order.append(k)
    parts = local_call(
        lambda *refs: query_kernel(rows, order, *refs),
        [shape((rows, features), jnp.float32)] * 4,
        len(pieces) + 2,
        6,
        scratch=[pltpu.VMEM((len(pieces) * rows, query_weight.shape[0]), jnp.float32)],
    )(place, *pieces, query_weight)
    arrived = [parts[0]] + [flipped(parts[k], k // 2, k % 2) for k in (1, 3, 2)]
    spread = local_call(
        lambda *refs: attend_kernel(narrow, *refs),
        shape((wide * narrow, rows, width // narrow), jnp.bfloat16),
        9,
        16,
    )(limit, route, *arrived, cache_keys, cache_values, output_weight)
    gathered = lax.all_to_all(spread, ("wide", "narrow"), 0, 0, tiled=True)
    return local_call(
        sum_kernel, shape((rows, width // narrow), jnp.bfloat16), 1, 1
    )(gathered)


def solution(mesh):
    placed = (
        P(("wide", "depth"), None),
        P("depth", "narrow"),
        P("narrow", None),
        P(("wide", "depth"), None, "narrow"),
        P(("wide", "depth"), None, "narrow"),
        P(),
        P(),
    )
    return jax.shard_map(
        shards,
        mesh=mesh,
        in_specs=placed,
        out_specs=P(("wide", "depth"), "narrow"),
        check_vma=False,
    )
```

```python
import jax
import jax.numpy as jnp
from jax import lax
from jax.experimental import pallas as pl
from jax.experimental.pallas import tpu as pltpu
from jax.sharding import PartitionSpec as P

HDIM = 64
BLOCK = 128
SUBLANES = 8
LANES = 128

MIB = 1 << 20
VMEM = pl.BlockSpec(memory_space=pltpu.VMEM)


def crossing(chip, flip_depth):
    return (chip & 1) ^ flip_depth


def norm_kernel(hidden_ref, own_ref, other_ref):
    half = own_ref.shape[1]
    at_depth = lax.axis_index("depth")
    widened = hidden_ref[...].astype(jnp.float32)
    mean_square = jnp.mean(widened * widened, axis=-1, keepdims=True)
    normed = widened * lax.rsqrt(mean_square + 1e-06)
    low, high = normed[:, :half], normed[:, half:]
    first = at_depth == 0
    own_ref[...] = jnp.where(first, low, high).astype(jnp.bfloat16)
    other_ref[...] = jnp.where(first, high, low).astype(jnp.bfloat16)


def table_kernel(sizes, slot_hbm, blocks_hbm, place_ref, limit_ref, route_ref, *scratch):
    wide, halves, rows = sizes
    slot_ref, blocks_ref, slot_sem, blocks_sem = scratch
    slot_copy = pltpu.make_async_copy(slot_hbm, slot_ref, slot_sem)
    blocks_copy = pltpu.make_async_copy(blocks_hbm, blocks_ref, blocks_sem)
    slot_copy.start()
    blocks_copy.start()
    slot_copy.wait()
    blocks_copy.wait()
    at_wide, at_depth = lax.axis_index("wide"), lax.axis_index("depth")
    total = slot_ref.shape[1]
    slots = slot_ref[...]

    def iota(count, dim):
        return lax.broadcasted_iota(jnp.int32, (count, total), dim)

    target = iota(SUBLANES, 0)
    peer = target // rows
    slot = ((at_wide ^ (peer // 2)) * halves + (at_depth ^ (peer % 2))) * rows + target % rows
    request = jnp.sum(jnp.where(slots == slot, iota(SUBLANES, 1), 0), axis=1, keepdims=True)
    from_wide = (request // (rows * halves)) ^ at_wide
    from_depth = (request // rows % halves) ^ at_depth
    place = ((from_wide >> 1) * halves + from_depth) * rows + request % rows
    here = (from_wide & 1) == crossing(from_wide >> 1, from_depth)
    place_ref[...] = jnp.broadcast_to(jnp.where(here, place, -1), place_ref.shape)
    base = (at_wide * halves + at_depth) * rows
    for j in range(rows):
        count = jnp.sum(jnp.where(slots == base + j, blocks_ref[...], 0), axis=1, keepdims=True)
        limit_ref[j] = jnp.broadcast_to(count * BLOCK, limit_ref.shape[1:])
    line = iota(wide * rows, 0)
    request = (line // rows * halves + at_depth) * rows + line % rows
    held = jnp.sum(jnp.where(iota(wide * rows, 1) == request, slots, 0), axis=1, keepdims=True)
    route_ref[...] = jnp.broadcast_to(held - base, route_ref.shape)


def turn_kernel(keys_ref, turned_ref):
    for j in range(keys_ref.shape[0]):
        turned_ref[j] = keys_ref[j].T


def query_kernel(rows, order, place_ref, *refs):
    pieces = len(refs) - 1 - 4 - 1
    piece_refs, weight_ref = refs[:pieces], refs[pieces]
    out_refs, rows_ref = refs[pieces + 1 : pieces + 5], refs[pieces + 5]
    for k, piece in zip(order, piece_refs):
        rows_ref[k * rows : (k + 1) * rows, :] = piece[...].astype(jnp.float32)
    sums = jnp.dot(
        rows_ref[...].astype(jnp.bfloat16), weight_ref[...], preferred_element_type=jnp.float32
    )
    place = place_ref[...]
    for c in range(sums.shape[1] // LANES):
        span = slice(c * LANES, (c + 1) * LANES)
        picked = jnp.zeros_like(place, jnp.float32)
        for g in range(sums.shape[0] // SUBLANES):
            lines = sums[g * SUBLANES : (g + 1) * SUBLANES, span]
            found = jnp.take_along_axis(lines, place & (SUBLANES - 1), axis=0)
            picked = jnp.where(place >> 3 == g, found, picked)
        for k, out in enumerate(out_refs):
            out[:, span] = picked[k * rows : (k + 1) * rows]


def attend_kernel(narrow, limit_ref, route_ref, *refs):
    parts, (keys_ref, values_ref, weight_ref, out_ref) = refs[:4], refs[4:]
    rows, features, cache_len = keys_ref.shape
    heads = features // HDIM
    queries = (parts[0][...] + parts[2][...]) + (parts[1][...] + parts[3][...])
    of_head = (
        lax.broadcasted_iota(jnp.int32, (heads, features), 1) // HDIM
        == lax.broadcasted_iota(jnp.int32, (heads, features), 0)
    )
    positions = lax.broadcasted_iota(jnp.int32, (heads, cache_len), 1)
    scores, shares, mixed = [], [], []
    for j in range(rows):
        spread = jnp.where(of_head, queries[j : j + 1, :], 0.0).astype(jnp.bfloat16)
        scores.append(
            jnp.dot(spread, keys_ref[j], preferred_element_type=jnp.float32)
        )
    for j in range(rows):
        masked = jnp.where(positions < limit_ref[j], scores[j], jnp.float32(-1e30))
        row_top = jnp.max(masked, axis=-1, keepdims=True)
        raised = jnp.exp(masked - row_top)
        shares.append((raised / jnp.sum(raised, axis=-1, keepdims=True)).astype(jnp.bfloat16))
    for j in range(rows):
        mixed.append(jnp.dot(shares[j], values_ref[j], preferred_element_type=jnp.float32))
    route = route_ref[...]
    context = jnp.zeros(route.shape, jnp.float32)
    for j in range(rows):
        line = jnp.sum(jnp.where(of_head, mixed[j], 0.0), axis=0, keepdims=True)
        context = jnp.where(route == j, line, context)
    partial = jnp.dot(
        context.astype(jnp.bfloat16), weight_ref[...], preferred_element_type=jnp.float32
    )
    width = partial.shape[1] // narrow
    for to_wide in range(partial.shape[0] // rows):
        block = partial[to_wide * rows : (to_wide + 1) * rows].astype(jnp.bfloat16)
        for to_narrow in range(narrow):
            out_ref[to_wide * narrow + to_narrow] = block[
                :, to_narrow * width : (to_narrow + 1) * width
            ]


def sum_kernel(parts_ref, out_ref):
    total = parts_ref[0].astype(jnp.float32)
    for k in range(1, parts_ref.shape[0]):
        total = total + parts_ref[k].astype(jnp.float32)
    out_ref[...] = total.astype(jnp.bfloat16)


def local_call(kernel, out_shape, count, mib, scratch=(), cost=None, spec=VMEM):
    several = isinstance(out_shape, list)
    return pl.pallas_call(
        kernel,
        out_shape=out_shape,
        in_specs=[spec] * count,
        out_specs=[VMEM] * len(out_shape) if several else VMEM,
        scratch_shapes=scratch,
        compiler_params=pltpu.CompilerParams(vmem_limit_bytes=mib * MIB),
        cost_estimate=cost,
    )


def cost_of(flops):
    return pl.CostEstimate(flops=flops, bytes_accessed=0, transcendentals=0)


def shards(
    hidden_state, query_weight, output_weight, cache_keys, cache_values, enc_blocks, cache_slot
):
    rows = hidden_state.shape[0]
    wide, narrow, halves = (lax.axis_size(name) for name in ("wide", "narrow", "depth"))
    features = query_weight.shape[1]
    cache_len = cache_keys.shape[1]
    width = output_weight.shape[1]

    def flipped(x, flip_wide, flip_depth):
        pairs = [
            (w * halves + d, (w ^ flip_wide) * halves + (d ^ flip_depth))
            for w in range(wide)
            for d in range(halves)
        ]
        return lax.ppermute(x, ("wide", "depth"), pairs)

    shape = jax.ShapeDtypeStruct
    place, limit, route = local_call(
        lambda *refs: table_kernel((wide, halves, rows), *refs),
        [
            shape((4 * rows, LANES), jnp.int32),
            shape((rows, features // HDIM, cache_len), jnp.int32),
            shape((wide * rows, features), jnp.int32),
        ],
        2,
        1,
        scratch=[
            pltpu.VMEM((1, cache_slot.shape[0]), jnp.int32),
            pltpu.VMEM((1, cache_slot.shape[0]), jnp.int32),
            pltpu.SemaphoreType.DMA(()),
            pltpu.SemaphoreType.DMA(()),
        ],
        cost=cost_of(10**9),
        spec=pl.BlockSpec(memory_space=pltpu.HBM),
    )(cache_slot[None], enc_blocks[None])
    half_rows = shape((rows, query_weight.shape[0]), jnp.bfloat16)
    own, other = local_call(norm_kernel, [half_rows, half_rows], 1, 1, cost=cost_of(5 * 10**9))(hidden_state)
    turned = local_call(
        turn_kernel,
        shape((rows, features, cache_len), jnp.bfloat16),
        1,
        6,
    )(cache_keys)
    pieces, order = [own], [0]
    for k in range(1, wide // 2 * halves):
        chip, flip_depth = k // halves, k % halves
        flip_wide = chip * 2 + crossing(chip, flip_depth)
        pieces.append(flipped(other if flip_depth else own, flip_wide, flip_depth))
        order.append(k)
    parts = local_call(
        lambda *refs: query_kernel(rows, order, *refs),
        [shape((rows, features), jnp.float32)] * 4,
        len(pieces) + 2,
        6,
        scratch=[pltpu.VMEM((len(pieces) * rows, query_weight.shape[0]), jnp.float32)],
    )(place, *pieces, query_weight)
    arrived = [parts[0]] + [flipped(parts[k], k // 2, k % 2) for k in (1, 3, 2)]
    spread = local_call(
        lambda *refs: attend_kernel(narrow, *refs),
        shape((wide * narrow, rows, width // narrow), jnp.bfloat16),
        9,
        16,
    )(limit, route, *arrived, turned, cache_values, output_weight)
    gathered = lax.all_to_all(spread, ("wide", "narrow"), 0, 0, tiled=True)
    return local_call(
        sum_kernel, shape((rows, width // narrow), jnp.bfloat16), 1, 1
    )(gathered)


def solution(mesh):
    placed = (
        P(("wide", "depth"), None),
        P("depth", "narrow"),
        P("narrow", None),
        P(("wide", "depth"), None, "narrow"),
        P(("wide", "depth"), None, "narrow"),
        P(),
        P(),
    )
    return jax.shard_map(
        shards,
        mesh=mesh,
        in_specs=placed,
        out_specs=P(("wide", "depth"), "narrow"),
        check_vma=False,
    )
```

```python
import jax
import jax.numpy as jnp
from jax import lax
from jax.experimental import pallas as pl
from jax.experimental.pallas import tpu as pltpu
from jax.sharding import PartitionSpec as P


HDIM = 64
BLOCK = 128
SUBLANES = 8
LANES = 128

MIB = 1 << 20
VMEM = pl.BlockSpec(memory_space=pltpu.VMEM)
HBM = pl.BlockSpec(memory_space=pltpu.HBM)


def crossing(chip, flip_depth):
    return (chip & 1) ^ flip_depth


def normed_halves(hidden_ref):
    half = hidden_ref.shape[1] // 2
    widened = hidden_ref[...].astype(jnp.float32)
    mean_square = jnp.mean(widened * widened, axis=-1, keepdims=True)
    normed = widened * lax.rsqrt(mean_square + 1e-06)
    low, high = normed[:, :half], normed[:, half:]
    first = lax.axis_index("depth") == 0
    own, other = jnp.where(first, low, high), jnp.where(first, high, low)
    return own.astype(jnp.bfloat16), other.astype(jnp.bfloat16)


def norm_kernel(hidden_ref, own_ref, other_ref):
    own_ref[...], other_ref[...] = normed_halves(hidden_ref)


def arrived_kernel(hidden_ref, own_ref):
    own_ref[...] = normed_halves(hidden_ref)[0]


def wanted_kernel(sizes, wanted_ref):
    halves, rows = sizes
    at_wide, at_depth = lax.axis_index("wide"), lax.axis_index("depth")
    target = lax.broadcasted_iota(jnp.int32, wanted_ref.shape, 0)
    peer = target // rows
    peer_at = (at_wide ^ (peer // 2)) * halves + (at_depth ^ (peer % 2))
    wanted_ref[...] = peer_at * rows + target % rows


def table_kernel(sizes, wanted_ref, slot_hbm, blocks_hbm, place_ref, limit_ref, route_ref, *scratch):
    wide, halves, rows = sizes
    slot_ref, blocks_ref, slot_sem, blocks_sem = scratch
    slot_copy = pltpu.make_async_copy(slot_hbm, slot_ref, slot_sem)
    blocks_copy = pltpu.make_async_copy(blocks_hbm, blocks_ref, blocks_sem)
    slot_copy.start()
    blocks_copy.start()
    slot_copy.wait()
    blocks_copy.wait()
    at_wide, at_depth = lax.axis_index("wide"), lax.axis_index("depth")
    total = slot_ref.shape[1]
    slots = slot_ref[...]

    def iota(count, dim):
        return lax.broadcasted_iota(jnp.int32, (count, total), dim)

    wanted = wanted_ref[...]
    request = jnp.sum(jnp.where(slots == wanted, iota(SUBLANES, 1), 0), axis=1, keepdims=True)
    from_wide = (request // (rows * halves)) ^ at_wide
    from_depth = (request // rows % halves) ^ at_depth
    place = ((from_wide >> 1) * halves + from_depth) * rows + request % rows
    here = (from_wide & 1) == crossing(from_wide >> 1, from_depth)
    place_ref[...] = jnp.broadcast_to(jnp.where(here, place, -1), place_ref.shape)
    base = (at_wide * halves + at_depth) * rows
    for j in range(rows):
        count = jnp.sum(jnp.where(slots == base + j, blocks_ref[...], 0), axis=1, keepdims=True)
        limit_ref[j] = jnp.broadcast_to(count * BLOCK, limit_ref.shape[1:])
    line = iota(wide * rows, 0)
    request = (line // rows * halves + at_depth) * rows + line % rows
    held = jnp.sum(jnp.where(iota(wide * rows, 1) == request, slots, 0), axis=1, keepdims=True)
    route_ref[...] = jnp.broadcast_to(held - base, route_ref.shape)


def turn_kernel(keys_ref, turned_ref):
    for j in range(keys_ref.shape[0]):
        turned_ref[j] = keys_ref[j].T


def query_kernel(rows, order, place_ref, *refs):
    pieces = len(refs) - 1 - 4 - 1
    piece_refs, weight_ref = refs[:pieces], refs[pieces]
    out_refs, rows_ref = refs[pieces + 1 : pieces + 5], refs[pieces + 5]
    for k, piece in zip(order, piece_refs):
        rows_ref[k * rows : (k + 1) * rows, :] = piece[...].astype(jnp.float32)
    sums = jnp.dot(
        rows_ref[...].astype(jnp.bfloat16), weight_ref[...], preferred_element_type=jnp.float32
    )
    place = place_ref[...]
    for c in range(sums.shape[1] // LANES):
        span = slice(c * LANES, (c + 1) * LANES)
        picked = jnp.zeros_like(place, jnp.float32)
        for g in range(sums.shape[0] // SUBLANES):
            lines = sums[g * SUBLANES : (g + 1) * SUBLANES, span]
            found = jnp.take_along_axis(lines, place & (SUBLANES - 1), axis=0)
            picked = jnp.where(place >> 3 == g, found, picked)
        for k, out in enumerate(out_refs):
            out[:, span] = picked[k * rows : (k + 1) * rows]


def attend_kernel(narrow, limit_ref, route_ref, *refs):
    parts, (keys_ref, values_ref, weight_ref, out_ref) = refs[:4], refs[4:]
    rows, features, cache_len = keys_ref.shape
    heads = features // HDIM
    queries = (parts[0][...] + parts[2][...]) + (parts[1][...] + parts[3][...])
    of_head = (
        lax.broadcasted_iota(jnp.int32, (heads, features), 1) // HDIM
        == lax.broadcasted_iota(jnp.int32, (heads, features), 0)
    )
    positions = lax.broadcasted_iota(jnp.int32, (heads, cache_len), 1)
    scores, shares, mixed = [], [], []
    for j in range(rows):
        spread = jnp.where(of_head, queries[j : j + 1, :], 0.0).astype(jnp.bfloat16)
        scores.append(
            jnp.dot(spread, keys_ref[j], preferred_element_type=jnp.float32)
        )
    for j in range(rows):
        masked = jnp.where(positions < limit_ref[j], scores[j], jnp.float32(-1e30))
        row_top = jnp.max(masked, axis=-1, keepdims=True)
        raised = jnp.exp(masked - row_top)
        shares.append((raised / jnp.sum(raised, axis=-1, keepdims=True)).astype(jnp.bfloat16))
    for j in range(rows):
        mixed.append(jnp.dot(shares[j], values_ref[j], preferred_element_type=jnp.float32))
    route = route_ref[...]
    context = jnp.zeros(route.shape, jnp.float32)
    for j in range(rows):
        line = jnp.sum(jnp.where(of_head, mixed[j], 0.0), axis=0, keepdims=True)
        context = jnp.where(route == j, line, context)
    partial = jnp.dot(
        context.astype(jnp.bfloat16), weight_ref[...], preferred_element_type=jnp.float32
    )
    width = partial.shape[1] // narrow
    for to_wide in range(partial.shape[0] // rows):
        block = partial[to_wide * rows : (to_wide + 1) * rows].astype(jnp.bfloat16)
        for to_narrow in range(narrow):
            out_ref[to_wide * narrow + to_narrow] = block[
                :, to_narrow * width : (to_narrow + 1) * width
            ]


def sum_kernel(parts_ref, out_ref):
    total = parts_ref[0].astype(jnp.float32)
    for k in range(1, parts_ref.shape[0]):
        total = total + parts_ref[k].astype(jnp.float32)
    out_ref[...] = total.astype(jnp.bfloat16)


def local_call(kernel, out_shape, count, mib, scratch=(), cost=None, far=0):
    several = isinstance(out_shape, list)
    return pl.pallas_call(
        kernel,
        out_shape=out_shape,
        in_specs=[VMEM] * (count - far) + [HBM] * far,
        out_specs=[VMEM] * len(out_shape) if several else VMEM,
        scratch_shapes=scratch,
        compiler_params=pltpu.CompilerParams(vmem_limit_bytes=mib * MIB),
        cost_estimate=cost,
    )


def cost_of(flops):
    return pl.CostEstimate(flops=flops, bytes_accessed=0, transcendentals=0)


def shards(
    hidden_state, query_weight, output_weight, cache_keys, cache_values, enc_blocks, cache_slot
):
    rows = hidden_state.shape[0]
    wide, narrow, halves = (lax.axis_size(name) for name in ("wide", "narrow", "depth"))
    features = query_weight.shape[1]
    cache_len = cache_keys.shape[1]
    width = output_weight.shape[1]

    def flipped(x, flip_wide, flip_depth):
        pairs = [
            (w * halves + d, (w ^ flip_wide) * halves + (d ^ flip_depth))
            for w in range(wide)
            for d in range(halves)
        ]
        return lax.ppermute(x, ("wide", "depth"), pairs)

    shape = jax.ShapeDtypeStruct
    wanted = local_call(
        lambda *refs: wanted_kernel((halves, rows), *refs),
        shape((4 * rows, cache_slot.shape[0]), jnp.int32),
        0,
        1,
        cost=cost_of(10**10),
    )()
    place, limit, route = local_call(
        lambda *refs: table_kernel((wide, halves, rows), *refs),
        [
            shape((4 * rows, LANES), jnp.int32),
            shape((rows, features // HDIM, cache_len), jnp.int32),
            shape((wide * rows, features), jnp.int32),
        ],
        3,
        1,
        scratch=[
            pltpu.VMEM((1, cache_slot.shape[0]), jnp.int32),
            pltpu.VMEM((1, cache_slot.shape[0]), jnp.int32),
            pltpu.SemaphoreType.DMA(()),
            pltpu.SemaphoreType.DMA(()),
        ],
        cost=cost_of(10**9),
        far=2,
    )(wanted, cache_slot[None], enc_blocks[None])
    half_rows = shape((rows, query_weight.shape[0]), jnp.bfloat16)
    own, other = local_call(
        norm_kernel, [half_rows, half_rows], 1, 1, cost=cost_of(5 * 10**9)
    )(hidden_state)
    turned = local_call(
        turn_kernel,
        shape((rows, features, cache_len), jnp.bfloat16),
        1,
        6,
    )(cache_keys)
    pieces, order = [own], [0]
    last = wide // 2 * halves - 1
    for k in range(1, last + 1):
        chip, flip_depth = k // halves, k % halves
        flip_wide = chip * 2 + crossing(chip, flip_depth)
        if k == last:
            raw = flipped(hidden_state, flip_wide, flip_depth)
            piece = local_call(arrived_kernel, half_rows, 1, 1)(raw)
        else:
            piece = flipped(other if flip_depth else own, flip_wide, flip_depth)
        pieces.append(piece)
        order.append(k)
    parts = local_call(
        lambda *refs: query_kernel(rows, order, *refs),
        [shape((rows, features), jnp.float32)] * 4,
        len(pieces) + 2,
        6,
        scratch=[pltpu.VMEM((len(pieces) * rows, query_weight.shape[0]), jnp.float32)],
    )(place, *pieces, query_weight)
    arrived = [parts[0]] + [flipped(parts[k], k // 2, k % 2) for k in (1, 3, 2)]
    spread = local_call(
        lambda *refs: attend_kernel(narrow, *refs),
        shape((wide * narrow, rows, width // narrow), jnp.bfloat16),
        9,
        16,
    )(limit, route, *arrived, turned, cache_values, output_weight)
    gathered = lax.all_to_all(spread, ("wide", "narrow"), 0, 0, tiled=True)
    return local_call(
        sum_kernel, shape((rows, width // narrow), jnp.bfloat16), 1, 1
    )(gathered)


def solution(mesh):
    placed = (
        P(("wide", "depth"), None),
        P("depth", "narrow"),
        P("narrow", None),
        P(("wide", "depth"), None, "narrow"),
        P(("wide", "depth"), None, "narrow"),
        P(),
        P(),
    )
    return jax.shard_map(
        shards,
        mesh=mesh,
        in_specs=placed,
        out_specs=P(("wide", "depth"), "narrow"),
        check_vma=False,
    )
```

```python
import jax
import jax.numpy as jnp
from jax import lax
from jax.experimental import pallas as pl
from jax.experimental.pallas import tpu as pltpu
from jax.sharding import PartitionSpec as P


HDIM = 64
BLOCK = 128
SUBLANES = 8
LANES = 128

MIB = 1 << 20
VMEM = pl.BlockSpec(memory_space=pltpu.VMEM)
HBM = pl.BlockSpec(memory_space=pltpu.HBM)


def crossing(chip, flip_depth):
    return (chip & 1) ^ flip_depth


def normed_halves(hidden_ref):
    half = hidden_ref.shape[1] // 2
    widened = hidden_ref[...].astype(jnp.float32)
    mean_square = jnp.mean(widened * widened, axis=-1, keepdims=True)
    normed = widened * lax.rsqrt(mean_square + 1e-06)
    low, high = normed[:, :half], normed[:, half:]
    first = lax.axis_index("depth") == 0
    own, other = jnp.where(first, low, high), jnp.where(first, high, low)
    return own.astype(jnp.bfloat16), other.astype(jnp.bfloat16)


def norm_kernel(hidden_ref, own_ref, other_ref):
    own_ref[...], other_ref[...] = normed_halves(hidden_ref)


def arrived_kernel(hidden_ref, own_ref):
    own_ref[...] = normed_halves(hidden_ref)[0]


def wanted_kernel(sizes, wanted_ref):
    halves, rows = sizes
    at_wide, at_depth = lax.axis_index("wide"), lax.axis_index("depth")
    target = lax.broadcasted_iota(jnp.int32, wanted_ref.shape, 0)
    peer = target // rows
    peer_at = (at_wide ^ (peer // 2)) * halves + (at_depth ^ (peer % 2))
    wanted_ref[...] = peer_at * rows + target % rows


def table_kernel(sizes, wanted_ref, slot_hbm, blocks_hbm, place_ref, limit_ref, route_ref, *scratch):
    wide, halves, rows = sizes
    slot_ref, blocks_ref, slot_sem, blocks_sem = scratch
    slot_copy = pltpu.make_async_copy(slot_hbm, slot_ref, slot_sem)
    blocks_copy = pltpu.make_async_copy(blocks_hbm, blocks_ref, blocks_sem)
    slot_copy.start()
    blocks_copy.start()
    slot_copy.wait()
    blocks_copy.wait()
    at_wide, at_depth = lax.axis_index("wide"), lax.axis_index("depth")
    total = slot_ref.shape[1]
    slots = slot_ref[...]

    def iota(count, dim):
        return lax.broadcasted_iota(jnp.int32, (count, total), dim)

    wanted = wanted_ref[...]
    request = jnp.sum(jnp.where(slots == wanted, iota(SUBLANES, 1), 0), axis=1, keepdims=True)
    from_wide = (request // (rows * halves)) ^ at_wide
    from_depth = (request // rows % halves) ^ at_depth
    place = ((from_wide >> 1) * halves + from_depth) * rows + request % rows
    here = (from_wide & 1) == crossing(from_wide >> 1, from_depth)
    place_ref[...] = jnp.broadcast_to(jnp.where(here, place, -1), place_ref.shape)
    base = (at_wide * halves + at_depth) * rows
    for j in range(rows):
        count = jnp.sum(jnp.where(slots == base + j, blocks_ref[...], 0), axis=1, keepdims=True)
        limit_ref[j] = jnp.broadcast_to(count * BLOCK, limit_ref.shape[1:])
    line = iota(wide * rows, 0)
    request = (line // rows * halves + at_depth) * rows + line % rows
    held = jnp.sum(jnp.where(iota(wide * rows, 1) == request, slots, 0), axis=1, keepdims=True)
    route_ref[...] = jnp.broadcast_to(held - base, route_ref.shape)


def turn_kernel(keys_ref, turned_ref):
    for j in range(keys_ref.shape[0]):
        turned_ref[j] = keys_ref[j].T


def query_kernel(rows, order, place_ref, *refs):
    pieces = len(refs) - 1 - 4 - 1
    piece_refs, weight_ref = refs[:pieces], refs[pieces]
    out_refs, rows_ref = refs[pieces + 1 : pieces + 5], refs[pieces + 5]
    for k, piece in zip(order, piece_refs):
        rows_ref[k * rows : (k + 1) * rows, :] = piece[...].astype(jnp.float32)
    sums = jnp.dot(
        rows_ref[...].astype(jnp.bfloat16), weight_ref[...], preferred_element_type=jnp.float32
    )
    place = place_ref[...]
    for c in range(sums.shape[1] // LANES):
        span = slice(c * LANES, (c + 1) * LANES)
        picked = jnp.zeros_like(place, jnp.float32)
        for g in range(sums.shape[0] // SUBLANES):
            lines = sums[g * SUBLANES : (g + 1) * SUBLANES, span]
            found = jnp.take_along_axis(lines, place & (SUBLANES - 1), axis=0)
            picked = jnp.where(place >> 3 == g, found, picked)
        for k, out in enumerate(out_refs):
            out[:, span] = picked[k * rows : (k + 1) * rows]


def attend_kernel(narrow, limit_ref, route_ref, *refs):
    parts, (keys_ref, values_ref, weight_ref, out_ref) = refs[:4], refs[4:]
    rows, features, cache_len = keys_ref.shape
    heads = features // HDIM
    queries = (parts[0][...] + parts[2][...]) + (parts[1][...] + parts[3][...])
    of_head = (
        lax.broadcasted_iota(jnp.int32, (heads, features), 1) // HDIM
        == lax.broadcasted_iota(jnp.int32, (heads, features), 0)
    )
    positions = lax.broadcasted_iota(jnp.int32, (heads, cache_len), 1)
    scores, shares, mixed = [], [], []
    for j in range(rows):
        spread = jnp.where(of_head, queries[j : j + 1, :], 0.0).astype(jnp.bfloat16)
        scores.append(
            jnp.dot(spread, keys_ref[j], preferred_element_type=jnp.float32)
        )
    for j in range(rows):
        masked = jnp.where(positions < limit_ref[j], scores[j], jnp.float32(-1e30))
        row_top = jnp.max(masked, axis=-1, keepdims=True)
        raised = jnp.exp(masked - row_top)
        shares.append((raised / jnp.sum(raised, axis=-1, keepdims=True)).astype(jnp.bfloat16))
    for j in range(rows):
        mixed.append(jnp.dot(shares[j], values_ref[j], preferred_element_type=jnp.float32))
    route = route_ref[...]
    context = jnp.zeros(route.shape, jnp.float32)
    for j in range(rows):
        line = jnp.sum(jnp.where(of_head, mixed[j], 0.0), axis=0, keepdims=True)
        context = jnp.where(route == j, line, context)
    context = context.astype(jnp.bfloat16)
    width = weight_ref.shape[1] // narrow
    for to_narrow in range(narrow):
        span = slice(to_narrow * width, (to_narrow + 1) * width)
        partial = jnp.dot(context, weight_ref[:, span], preferred_element_type=jnp.float32)
        for to_wide in range(partial.shape[0] // rows):
            block = partial[to_wide * rows : (to_wide + 1) * rows]
            out_ref[to_wide * narrow + to_narrow] = block.astype(jnp.bfloat16)


def sum_kernel(parts_ref, out_ref):
    total = parts_ref[0].astype(jnp.float32)
    for k in range(1, parts_ref.shape[0]):
        total = total + parts_ref[k].astype(jnp.float32)
    out_ref[...] = total.astype(jnp.bfloat16)


def local_call(kernel, out_shape, count, mib, scratch=(), cost=None, far=0):
    several = isinstance(out_shape, list)
    return pl.pallas_call(
        kernel,
        out_shape=out_shape,
        in_specs=[VMEM] * (count - far) + [HBM] * far,
        out_specs=[VMEM] * len(out_shape) if several else VMEM,
        scratch_shapes=scratch,
        compiler_params=pltpu.CompilerParams(vmem_limit_bytes=mib * MIB),
        cost_estimate=cost,
    )


def cost_of(flops):
    return pl.CostEstimate(flops=flops, bytes_accessed=0, transcendentals=0)


def shards(
    hidden_state, query_weight, output_weight, cache_keys, cache_values, enc_blocks, cache_slot
):
    rows = hidden_state.shape[0]
    wide, narrow, halves = (lax.axis_size(name) for name in ("wide", "narrow", "depth"))
    features = query_weight.shape[1]
    cache_len = cache_keys.shape[1]
    width = output_weight.shape[1]

    def flipped(x, flip_wide, flip_depth):
        pairs = [
            (w * halves + d, (w ^ flip_wide) * halves + (d ^ flip_depth))
            for w in range(wide)
            for d in range(halves)
        ]
        return lax.ppermute(x, ("wide", "depth"), pairs)

    shape = jax.ShapeDtypeStruct
    wanted = local_call(
        lambda *refs: wanted_kernel((halves, rows), *refs),
        shape((4 * rows, cache_slot.shape[0]), jnp.int32),
        0,
        1,
        cost=cost_of(10**10),
    )()
    place, limit, route = local_call(
        lambda *refs: table_kernel((wide, halves, rows), *refs),
        [
            shape((4 * rows, LANES), jnp.int32),
            shape((rows, features // HDIM, cache_len), jnp.int32),
            shape((wide * rows, features), jnp.int32),
        ],
        3,
        1,
        scratch=[
            pltpu.VMEM((1, cache_slot.shape[0]), jnp.int32),
            pltpu.VMEM((1, cache_slot.shape[0]), jnp.int32),
            pltpu.SemaphoreType.DMA(()),
            pltpu.SemaphoreType.DMA(()),
        ],
        cost=cost_of(10**9),
        far=2,
    )(wanted, cache_slot[None], enc_blocks[None])
    half_rows = shape((rows, query_weight.shape[0]), jnp.bfloat16)
    own, other = local_call(
        norm_kernel, [half_rows, half_rows], 1, 1, cost=cost_of(5 * 10**9)
    )(hidden_state)
    turned = local_call(
        turn_kernel,
        shape((rows, features, cache_len), jnp.bfloat16),
        1,
        6,
    )(cache_keys)
    pieces, order = [own], [0]
    last = wide // 2 * halves - 1
    for k in range(1, last + 1):
        chip, flip_depth = k // halves, k % halves
        flip_wide = chip * 2 + crossing(chip, flip_depth)
        if k == last:
            raw = flipped(hidden_state, flip_wide, flip_depth)
            piece = local_call(arrived_kernel, half_rows, 1, 1)(raw)
        else:
            piece = flipped(other if flip_depth else own, flip_wide, flip_depth)
        pieces.append(piece)
        order.append(k)
    parts = local_call(
        lambda *refs: query_kernel(rows, order, *refs),
        [shape((rows, features), jnp.float32)] * 4,
        len(pieces) + 2,
        6,
        scratch=[pltpu.VMEM((len(pieces) * rows, query_weight.shape[0]), jnp.float32)],
    )(place, *pieces, query_weight)
    arrived = [parts[0]] + [flipped(parts[k], k // 2, k % 2) for k in (1, 3, 2)]
    spread = local_call(
        lambda *refs: attend_kernel(narrow, *refs),
        shape((wide * narrow, rows, width // narrow), jnp.bfloat16),
        9,
        16,
    )(limit, route, *arrived, turned, cache_values, output_weight)
    gathered = lax.all_to_all(spread, ("wide", "narrow"), 0, 0, tiled=True)
    return local_call(
        sum_kernel, shape((rows, width // narrow), jnp.bfloat16), 1, 1
    )(gathered)


def solution(mesh):
    placed = (
        P(("wide", "depth"), None),
        P("depth", "narrow"),
        P("narrow", None),
        P(("wide", "depth"), None, "narrow"),
        P(("wide", "depth"), None, "narrow"),
        P(),
        P(),
    )
    return jax.shard_map(
        shards,
        mesh=mesh,
        in_specs=placed,
        out_specs=P(("wide", "depth"), "narrow"),
        check_vma=False,
    )
```
